32 devices in a mesh: groups: 2 (over x), lon: 16 (over z, y, core).
Axes of the slice: x: 2, y: 2, z: 4, core: 2. Of those that a mesh axis runs over, the one named last changes fastest.
Arguments:
- tracers: bfloat16 [2048, 64, 256], P(('groups', 'lon')), parts along dimension 0, may hold values from -6 to 6
- wind_fields: bfloat16 [2048, 64, 128], P(('groups', 'lon')), parts along dimension 0, may hold values from -3 to 3
- departures: int32 [32, 16, 2], P(('groups', 'lon')), parts along dimension 0, may hold values from -4 to 3, as said below
Outputs:
- advected: bfloat16 [2048, 64, 256], P(('groups', 'lon')), parts along dimension 0
The draws below stay inside these ranges and needn't reach their ends.
There are 2 independent parts, one for each index of `groups`. The reference program is written for one: setup_inputs(seed, part) draws one part's arguments, and reference() takes and returns one part's arrays. A program takes and returns all parts, laid end to end along the dimension named above; each array names one. Nothing has to cross between parts.
Inputs may be any that keep to these rules, and one draw needn't show every extreme that they name: `departures`: entry 0 lies in -4..3 and entry 1 in -1..1 with q - entry 1 a valid band; in every sector exactly 4 bands share one value of entry 0, and no value is shared by more.
All inputs are finite; a program needn't handle non-finite values.
Results may differ from the reference program's by a relative error of at most 0.001.
Values may be sent and summed in bfloat16 or wider, within the bound.
No kernel may reach another device: no remote copies, remote signals or barrier semaphores. Data moves between devices by JAX's collectives and lax.ppermute only.
A program may use at most 128 MiB of HBM per device.

```python
import jax
import jax.numpy as jnp
from jax import lax

NTRACER = 8
LEVELS = 32
CLON = 64
BR = 4
NB = 16
CAP = 4
TRAJ = 3
NLON = 1024
NLAT = 64
TCH = 256
N_LON = 16


def draw_departures(key, part):
    base_key = jax.random.fold_in(key, 7)
    sector_key, lat_key = jax.random.split(base_key, 2)

    def sector_draw(key_sector):
        first_key, second_key, third_key = jax.random.split(key_sector, 3)
        ordering = jax.random.permutation(first_key, jnp.arange(8, dtype=jnp.int32))
        remaining = jnp.repeat(ordering[1:], CAP - 1)
        remaining = jax.random.permutation(second_key, remaining)
        chosen = jnp.concatenate([jnp.full((CAP,), ordering[0], jnp.int32), remaining[:NB - CAP]])
        chosen = jax.random.permutation(third_key, chosen)
        return chosen - 4
    lon_tiles = jax.vmap(sector_draw)(jax.random.split(sector_key, N_LON))
    band_ids = jnp.arange(NB, dtype=jnp.int32)[None, :]
    lat_tiles = jax.random.randint(lat_key, (N_LON, NB), -1, 2, dtype=jnp.int32)
    lat_tiles = jnp.clip(lat_tiles, band_ids - NB + 1, band_ids)
    return jnp.stack([lon_tiles, lat_tiles], -1).astype(jnp.int32)


def level_of(own_key, shape, pieces, least, top_value):
    def one(axis_at, shards_of):
        heights = jax.random.uniform(jax.random.fold_in(jax.random.fold_in(own_key, 6), axis_at), (shards_of,), jnp.float32, least / len(pieces), top_value / len(pieces))
        return jnp.repeat(jnp.exp(heights), shape[axis_at] // shards_of).reshape((-1,) + (1,) * (len(shape) - axis_at - 1))

    factor_of = one(*pieces[0])
    for cut in pieces[1:]:
        factor_of = factor_of * one(*cut)
    return factor_of


def scatter_about(rng, extent, deviation, limit, cuts=(), kind=jnp.bfloat16):
    values = jax.random.normal(rng, extent, jnp.float32) * deviation
    if len(cuts) > 0:
        values = level_of(rng, extent, cuts, -0.22, 0.18) * values
    return jnp.clip(values, min=-limit, max=limit).astype(kind)


def setup_inputs(seed: int = 0, part: int = 0) -> dict:
    streams_of = jax.random.split(jax.random.key(seed), 4)
    part_keys = jax.random.split(jax.random.fold_in(streams_of[3], part), 4)
    tracers = scatter_about(part_keys[0], (NLON, NLAT, TCH), 1.0, 6.0, ((0, 16),))
    wind_fields = scatter_about(part_keys[1], (NLON, NLAT, 4 * LEVELS), 0.5, 3.0, ((0, 16),))
    departures = draw_departures(jax.random.fold_in(jax.random.fold_in(streams_of[3], part), 71), part)
    return {"tracers": tracers, "wind_fields": wind_fields, "departures": departures}


CLIP_BOUND = 0.95


def linear_kernel(distance):
    return jnp.maximum(1.0 - jnp.abs(distance), 0.0)


def cubic_kernel(distance):
    magnitude = jnp.abs(distance)
    inner_part = 0.5 * (1.0 - magnitude) * (2.0 - magnitude) * (1.0 + magnitude)
    outer_part = -(magnitude - 1.0) * (2.0 - magnitude) * (3.0 - magnitude) / 6.0
    return jnp.where(magnitude < 1.0, inner_part, jnp.where(magnitude < 2.0, outer_part, 0.0))


def advect_tile(source_tile, arrival_wind):
    columns = source_tile.shape[0] - 4
    band_rows = source_tile.shape[1] - 4
    levels = arrival_wind.shape[-1] // 2
    tracer_ch = source_tile.shape[-1] - 4 * levels
    per_level = tracer_ch // levels
    wind_data = source_tile[:, :, tracer_ch:].astype(jnp.float32)
    extrapolated = 2.0 * wind_data[:, :, :2 * levels] - wind_data[:, :, 2 * levels:]
    wind_here = arrival_wind.astype(jnp.float32)
    displace = jnp.clip(wind_here, -CLIP_BOUND, CLIP_BOUND)
    for iteration in range(TRAJ):
        lon_shift = displace[:, :, :levels]
        lat_shift = displace[:, :, levels:]
        accumulated = jnp.zeros_like(wind_here)
        for lat_step in (-1, 0, 1):
            lat_weight = linear_kernel(lat_step + lat_shift)
            for lon_step in (-1, 0, 1):
                weight = linear_kernel(lon_step + lon_shift) * lat_weight
                window = extrapolated[2 + lon_step:2 + lon_step + columns, 2 + lat_step:2 + lat_step + band_rows, :]
                accumulated = accumulated + jnp.concatenate([weight, weight], -1) * window
        displace = jnp.clip(0.5 * (wind_here + accumulated), -CLIP_BOUND, CLIP_BOUND)
    lon_shift = displace[:, :, :levels]
    lat_shift = displace[:, :, levels:]
    result = jnp.zeros((columns, band_rows, tracer_ch), jnp.float32)
    for lat_step in range(-2, 3):
        lat_dist = lat_step + lat_shift
        lat_weight = cubic_kernel(lat_dist)
        inner_rows = jnp.abs(lat_dist) < 1.0
        for lon_step in range(-2, 3):
            lon_dist = lon_step + lon_shift
            lon_weight = jnp.where(inner_rows, cubic_kernel(lon_dist), linear_kernel(lon_dist))
            weight = jnp.repeat(lon_weight * lat_weight, per_level, axis=-1)
            window = source_tile[2 + lon_step:2 + lon_step + columns, 2 + lat_step:2 + lat_step + band_rows, :tracer_ch]
            result = result + weight * window.astype(jnp.float32)
    return result.astype(jnp.bfloat16)


def reference(tracers, wind_fields, departures):
    combined = jnp.concatenate([tracers, wind_fields], -1)
    padded = jnp.concatenate([combined[:, :1], combined[:, :1], combined, combined[:, -1:], combined[:, -1:]], 1)
    padded = jnp.concatenate([padded[-2:], padded, padded[:2]], 0)
    channels = combined.shape[-1]

    def advect_one(tile_index):
        sector = tile_index // NB
        band_index = tile_index % NB
        lon_tiles = departures[sector, band_index, 0]
        lat_tiles = departures[sector, band_index, 1]
        source = ((sector - lon_tiles) % N_LON).astype(jnp.int32)
        source_band = (band_index - lat_tiles).astype(jnp.int32)
        zero_index = jnp.zeros((), jnp.int32)
        source_tile = lax.dynamic_slice(padded, (source * CLON, source_band * BR, zero_index), (CLON + 4, BR + 4, channels))
        arrival_wind = lax.dynamic_slice(wind_fields, (sector * CLON, band_index * BR, zero_index), (CLON, BR, 2 * LEVELS))
        return advect_tile(source_tile, arrival_wind)

    moved = lax.map(advect_one, jnp.arange(N_LON * NB, dtype=jnp.int32))
    moved = moved.reshape(N_LON, NB, CLON, BR, LEVELS * NTRACER)
    moved = jnp.transpose(moved, (0, 2, 1, 3, 4))
    return moved.reshape(N_LON * CLON, NB * BR, LEVELS * NTRACER)
```

```python
import functools

import jax
import jax.numpy as jnp
from jax import lax
from jax.experimental import pallas as pl
from jax.experimental.pallas import tpu as pltpu
from jax.sharding import PartitionSpec as P

CAP = 4
TRAJ = 3
FIRST = -4
LAST = 4
RIM = 2
LANES = 128
META = 16
CLIP_BOUND = 0.95
F32 = jnp.float32
BF16 = jnp.bfloat16


def shifted(block, axis, distance):
    count = lax.axis_size(axis)
    route = [((i - distance) % count, i) for i in range(count)]
    return lax.ppermute(block, axis, route)


def fill_slots(dep_ref, slot_ref, count_ref, bands):
    for offset in range(LAST - FIRST):
        count_ref[offset] = 0
        for slot in range(CAP):
            slot_ref[offset * CAP + slot] = -1

    def place(band, carry):
        offset = dep_ref[0, band, 0] - FIRST
        ordinal = count_ref[offset]
        slot_ref[offset * CAP + ordinal] = band
        count_ref[offset] = ordinal + 1
        return carry

    lax.fori_loop(0, bands, place, 0)


def wind_kernel(sizes, dep_ref, wind_ref, perm_ref, *rest):
    columns, rows, groups, inner, bands, band_rows = sizes
    outs = rest[: LAST - FIRST]
    wide_ref, here_ref, slot_ref, count_ref = rest[LAST - FIRST :]

    def widen(column, carry):
        wide_ref[pl.ds(column * rows, rows), :] = wind_ref[column].astype(F32)
        return carry

    lax.fori_loop(0, columns, widen, 0)
    fill_slots(dep_ref, slot_ref, count_ref, bands)
    perm = perm_ref[:, : 2 * LANES]

    def eight_rows(block, carry):
        parts = []
        for row in range(8):
            parts.append(
                jnp.concatenate(
                    [
                        wide_ref[pl.ds(g * inner * rows + block * 8 + row, inner, stride=rows), :]
                        for g in range(groups)
                    ],
                    axis=1,
                )
            )
        left = jnp.concatenate(parts, axis=0).astype(BF16)
        moved = jnp.dot(left, perm, preferred_element_type=F32)
        for comp in range(2):
            here_ref[comp, pl.ds(block * 8, 8)] = (
                moved[:, comp * LANES : (comp + 1) * LANES].reshape(8, inner, LANES).astype(BF16)
            )
        return carry

    lax.fori_loop(0, rows // 8, eight_rows, 0)
    lane = lax.broadcasted_iota(jnp.int32, (META, LANES), 1)
    size = band_rows * inner
    for offset in range(LAST - FIRST):
        meta = jnp.full((META, LANES), -1.0, F32)
        for slot in range(CAP):
            band = slot_ref[offset * CAP + slot]
            safe = jnp.maximum(band, 0)
            source = jnp.where(band >= 0, safe - dep_ref[0, safe, 1], -1)
            meta = jnp.where(lane == slot, source.astype(F32), meta)
            for comp in range(2):
                outs[offset][pl.ds((slot * 2 + comp) * size, size), :] = here_ref[
                    comp, pl.ds(safe * band_rows, band_rows)
                ].reshape(size, LANES)
        outs[offset][pl.ds(CAP * 2 * size, META), :] = meta.astype(BF16)


def prepare_kernel(
    sizes,
    tracers_ref,
    wind_ref,
    low_t_ref,
    high_t_ref,
    low_w_ref,
    high_w_ref,
    perm_ref,
    perm_w_ref,
    out_t_ref,
    out_e_ref,
    wide_t_ref,
    wide_w_ref,
    stage_t_ref,
    stage_e_ref,
    edge_t_ref,
    edge_e_ref,
    sem_ref,
    edge_sem_ref,
):
    columns, rows, groups, inner, padded_inner, per_level = sizes
    halves = tracers_ref.shape[-1] // LANES
    blocks = rows // 8

    def put(column, t_value, w_value):
        at = pl.ds(column * rows, rows)
        for half in range(halves):
            wide_t_ref[half, at, :] = t_value[:, half * LANES : (half + 1) * LANES].astype(F32)
        wide_w_ref[at, :] = w_value.astype(F32)

    def own(column, carry):
        put(column + RIM, tracers_ref[column], wind_ref[column])
        return carry

    lax.fori_loop(0, columns, own, 0)
    for column in range(RIM):
        put(column, low_t_ref[column], low_w_ref[column])
        put(columns + RIM + column, high_t_ref[column], high_w_ref[column])
    for column in range(columns + 2 * RIM, (groups - 1) * inner + padded_inner):
        at = pl.ds(column * rows, rows)
        for half in range(halves):
            wide_t_ref[half, at, :] = jnp.zeros((rows, LANES), F32)
        wide_w_ref[at, :] = jnp.zeros((rows, LANES), F32)

    def copies(block, slot):
        at = pl.ds(RIM + block * 8, 8)
        return (
            pltpu.make_async_copy(stage_t_ref.at[slot], out_t_ref.at[:, at], sem_ref.at[slot, 0]),
            pltpu.make_async_copy(stage_e_ref.at[slot], out_e_ref.at[:, at], sem_ref.at[slot, 1]),
        )

    def edge_copies(side):
        at = pl.ds(side * (rows + RIM), RIM)
        return (
            pltpu.make_async_copy(
                edge_t_ref.at[side], out_t_ref.at[:, at], edge_sem_ref.at[side, 0]
            ),
            pltpu.make_async_copy(
                edge_e_ref.at[side], out_e_ref.at[:, at], edge_sem_ref.at[side, 1]
            ),
        )

    def eight_rows(block, carry):
        slot = lax.rem(block, 2)

        @pl.when(block >= 2)
        def _():
            for copy in copies(block - 2, slot):
                copy.wait()

        parts_t = []
        parts_w = []
        for row in range(8):
            pieces_t = []
            pieces_w = []
            for g in range(groups):
                at = pl.ds(g * inner * rows + block * 8 + row, padded_inner, stride=rows)
                for half in range(halves):
                    pieces_t.append(wide_t_ref[half, at, :])
                pieces_w.append(wide_w_ref[at, :])
            parts_t.append(jnp.concatenate(pieces_t, axis=1))
            parts_w.append(jnp.concatenate(pieces_w, axis=1))
        left_t = jnp.concatenate(parts_t, axis=0).astype(BF16)
        left_w = jnp.concatenate(parts_w, axis=0).astype(BF16)
        moved_w = jnp.dot(left_w, perm_w_ref[...], preferred_element_type=F32)
        for comp in range(2):
            now = moved_w[:, comp * LANES : (comp + 1) * LANES]
            before = moved_w[:, (comp + 2) * LANES : (comp + 3) * LANES]
            stage_e_ref[slot, comp] = (2.0 * now - before).reshape(8, padded_inner, LANES)
        moved_t = lax.dot_general(
            left_t, perm_ref[...], (((1,), (1,)), ((), ())), preferred_element_type=F32
        )
        for tracer in range(per_level):
            stage_t_ref[slot, tracer] = moved_t[:, tracer * LANES : (tracer + 1) * LANES].reshape(
                8, padded_inner, LANES
            )
        for copy in copies(block, slot):
            copy.start()

        for side, which, row in ((0, 0, 0), (1, blocks - 1, 7)):

            @pl.when(block == which)
            def _():
                for repeat in range(RIM):
                    for tracer in range(per_level):
                        edge_t_ref[side, tracer, repeat] = stage_t_ref[slot, tracer, row]
                    for comp in range(2):
                        edge_e_ref[side, comp, repeat] = stage_e_ref[slot, comp, row]
                for copy in edge_copies(side):
                    copy.start()

        return carry

    lax.fori_loop(0, blocks, eight_rows, 0)
    for block in range(max(blocks - 2, 0), blocks):
        for copy in copies(block, block % 2):
            copy.wait()
    for side in range(2):
        for copy in edge_copies(side):
            copy.wait()


def cubic_weights(shift):
    e = jnp.abs(shift)
    positive = shift > 0.0
    one_less = 1.0 - e
    one_more = 1.0 + e
    two_less = 2.0 - e
    center = 0.5 * one_less * two_less * one_more
    near = 0.5 * e * two_less * one_more
    across = e * one_less * (-1.0 / 6.0)
    beyond = across * two_less
    far = across * one_more
    zero = jnp.zeros_like(e)
    return (
        jnp.where(positive, far, zero),
        jnp.where(positive, near, beyond),
        center,
        jnp.where(positive, beyond, near),
        jnp.where(positive, zero, far),
    ), positive


def linear_weights(shift):
    return jnp.maximum(shift, 0.0), 1.0 - jnp.abs(shift), jnp.maximum(-shift, 0.0)


def clipped(value):
    return jnp.clip(value, -CLIP_BOUND, CLIP_BOUND)


def advect_kernel(
    sizes,
    msg_ref,
    fields_ref,
    extra_ref,
    perm_hbm_ref,
    out_ref,
    t_ref,
    e_ref,
    perm_ref,
    result_ref,
    source_ref,
    sem_ref,
    perm_sem_ref,
):
    inner, band_rows, per_level = sizes
    size = band_rows * inner
    perm_copy = pltpu.make_async_copy(perm_hbm_ref, perm_ref, perm_sem_ref)
    perm_copy.start()
    meta = msg_ref[pl.ds(CAP * 2 * size, META), :].astype(F32)
    lane = lax.broadcasted_iota(jnp.int32, (META, LANES), 1)

    def copies(slot, source):
        at = pl.ds(source * band_rows, band_rows + 2 * RIM)
        return (
            pltpu.make_async_copy(extra_ref.at[:, at], e_ref.at[slot], sem_ref.at[slot, 0]),
            pltpu.make_async_copy(fields_ref.at[:, at], t_ref.at[slot], sem_ref.at[slot, 1]),
        )

    for slot in range(CAP):
        source = jnp.max(jnp.where(lane == slot, meta, -1.0)).astype(jnp.int32)
        source_ref[slot] = source

        @pl.when(source >= 0)
        def _():
            for copy in copies(slot, source):
                copy.start()

    def one_slot(slot, carry):
        source = source_ref[slot]

        @pl.when(source < 0)
        def _():
            result_ref[pl.ds(slot * size, size), :] = jnp.zeros((size, per_level * LANES), F32)

        @pl.when(source >= 0)
        def _():
            for copy in copies(slot, source):
                copy.wait()

            def one_row(row, inner_carry):
                here = [
                    msg_ref[pl.ds((slot * 2 + comp) * size + row * inner, inner), :].astype(F32)
                    for comp in range(2)
                ]
                for eight in range(inner // 8):
                    base = eight * 8
                    wind = [h[base : base + 8] for h in here]
                    window = [
                        [
                            [
                                e_ref[slot, comp, row + RIM + b, pl.ds(base + RIM + a, 8), :]
                                for a in (-1, 0, 1)
                            ]
                            for b in (-1, 0, 1)
                        ]
                        for comp in range(2)
                    ]
                    shift = [clipped(w) for w in wind]
                    for _ in range(TRAJ):
                        lon = linear_weights(shift[0])
                        lat = linear_weights(shift[1])
                        moved = []
                        for comp in range(2):
                            total = None
                            for b in range(3):
                                line = (
                                    lon[0] * window[comp][b][0]
                                    + lon[1] * window[comp][b][1]
                                    + lon[2] * window[comp][b][2]
                                )
                                line = lat[b] * line
                                total = line if total is None else total + line
                            moved.append(clipped(0.5 * (wind[comp] + total)))
                        shift = moved
                    lon_cubic, _ = cubic_weights(shift[0])
                    lat_cubic, north = cubic_weights(shift[1])
                    low, mid, high = linear_weights(shift[0])
                    zero = jnp.zeros_like(low)
                    lon_linear = (zero, low, mid, high, zero)
                    taps = []
                    for b in range(-2, 3):
                        for a in range(-2, 3):
                            if abs(b) == 2:
                                if abs(a) == 2:
                                    continue
                                weight = lon_linear[a + 2]
                            elif b == 0:
                                weight = lon_cubic[a + 2]
                            elif b == -1:
                                weight = jnp.where(north, lon_cubic[a + 2], lon_linear[a + 2])
                            else:
                                weight = jnp.where(north, lon_linear[a + 2], lon_cubic[a + 2])
                            taps.append((a, b, weight * lat_cubic[b + 2]))
                    for tracer in range(per_level):
                        total = None
                        for a, b, weight in taps:
                            term = weight * t_ref[
                                slot, tracer, row + RIM + b, pl.ds(base + RIM + a, 8), :
                            ]
                            total = term if total is None else total + term
                        result_ref[
                            pl.ds(slot * size + row * inner + base, 8),
                            tracer * LANES : (tracer + 1) * LANES,
                        ] = total
                return inner_carry

            lax.fori_loop(0, band_rows, one_row, 0)

        return carry

    lax.fori_loop(0, CAP, one_slot, 0)
    perm_copy.wait()
    out_ref[...] = jnp.dot(
        result_ref[...].astype(BF16), perm_ref[...], preferred_element_type=F32
    ).astype(BF16)


def gather_kernel(sizes, dep_ref, *rest):
    columns, rows, groups, inner, bands, band_rows = sizes
    ins = rest[: LAST - FIRST]
    out_ref, wide_ref, slot_ref, count_ref = rest[LAST - FIRST :]
    halves = out_ref.shape[-1] // LANES
    size = band_rows * inner
    fill_slots(dep_ref, slot_ref, count_ref, bands)
    for offset in range(LAST - FIRST):

        def one_slot(slot, carry):
            band = slot_ref[offset * CAP + slot]

            @pl.when(band >= 0)
            def _():
                for row in range(band_rows):
                    value = ins[offset][pl.ds(slot * size + row * inner, inner), :].astype(F32)
                    for g in range(groups):
                        at = pl.ds(g * inner * rows + band * band_rows + row, inner, stride=rows)
                        for half in range(halves):
                            first = (g * halves + half) * LANES
                            wide_ref[half, at, :] = value[:, first : first + LANES]

            return carry

        lax.fori_loop(0, CAP, one_slot, 0)

    def narrow(column, carry):
        at = pl.ds(column * rows, rows)
        for half in range(halves):
            out_ref[column, :, half * LANES : (half + 1) * LANES] = wide_ref[half, at, :].astype(
                BF16
            )
        return carry

    lax.fori_loop(0, columns, narrow, 0)


def one_hot(target, width):
    return (target[:, None] == jnp.arange(width, dtype=jnp.int32)[None, :]).astype(BF16)


def on_device(tracers, wind_fields, departures):
    columns, rows, tracer_ch = tracers.shape
    wind_ch = wind_fields.shape[-1]
    levels = wind_ch // 4
    per_level = tracer_ch // levels
    bands = departures.shape[1]
    band_rows = rows // bands
    groups = LANES // levels
    inner = columns // groups
    padded_inner = -(-(inner + 2 * RIM) // 8) * 8
    size = band_rows * inner
    offsets = LAST - FIRST
    wide = per_level * LANES

    index = jnp.arange(wide, dtype=jnp.int32)
    tracer, group, level = index // LANES, (index // levels) % groups, index % levels
    perm = one_hot(group * tracer_ch + level * per_level + tracer, wide)
    index = jnp.arange(groups * wind_ch, dtype=jnp.int32)
    group, kind, level = index // wind_ch, (index // levels) % 4, index % levels
    perm_w = one_hot(kind * LANES + group * levels + level, 4 * LANES)

    low_t = shifted(tracers[columns - RIM :], "lon", 1)
    high_t = shifted(tracers[:RIM], "lon", -1)
    low_w = shifted(wind_fields[columns - RIM :], "lon", 1)
    high_w = shifted(wind_fields[:RIM], "lon", -1)

    vmem = pl.BlockSpec(memory_space=pltpu.VMEM)
    smem = pl.BlockSpec(memory_space=pltpu.SMEM)
    anywhere = pl.BlockSpec(memory_space=pl.ANY)
    msg_shape = jax.ShapeDtypeStruct((CAP * 2 * size + META, LANES), BF16)
    tables = [pltpu.SMEM((offsets * CAP,), jnp.int32), pltpu.SMEM((offsets,), jnp.int32)]
    messages = pl.pallas_call(
        functools.partial(wind_kernel, (columns, rows, groups, inner, bands, band_rows)),
        out_shape=[msg_shape] * offsets,
        in_specs=[smem, vmem, vmem],
        out_specs=[vmem] * offsets,
        scratch_shapes=[
            pltpu.VMEM((columns * rows, LANES), F32),
            pltpu.VMEM((2, rows, inner, LANES), BF16),
        ]
        + tables,
        cost_estimate=pl.CostEstimate(flops=4_000_000, bytes_accessed=3_000_000, transcendentals=0),
        name="winds",
    )(departures, wind_fields, perm_w)

    arrived = [
        msg if FIRST + n == 0 else shifted(msg, "lon", -(FIRST + n))
        for n, msg in enumerate(messages)
    ]

    all_columns = (groups - 1) * inner + padded_inner
    fields, extra = pl.pallas_call(
        functools.partial(
            prepare_kernel, (columns, rows, groups, inner, padded_inner, per_level)
        ),
        out_shape=[
            jax.ShapeDtypeStruct((per_level, rows + 2 * RIM, padded_inner, LANES), F32),
            jax.ShapeDtypeStruct((2, rows + 2 * RIM, padded_inner, LANES), F32),
        ],
        in_specs=[vmem] * 8,
        out_specs=[anywhere] * 2,
        scratch_shapes=[
            pltpu.VMEM((tracer_ch // LANES, all_columns * rows, LANES), F32),
            pltpu.VMEM((all_columns * rows, LANES), F32),
            pltpu.VMEM((2, per_level, 8, padded_inner, LANES), F32),
            pltpu.VMEM((2, 2, 8, padded_inner, LANES), F32),
            pltpu.VMEM((2, per_level, RIM, padded_inner, LANES), F32),
            pltpu.VMEM((2, 2, RIM, padded_inner, LANES), F32),
            pltpu.SemaphoreType.DMA((2, 2)),
            pltpu.SemaphoreType.DMA((2, 2)),
        ],
        cost_estimate=pl.CostEstimate(
            flops=16_000_000, bytes_accessed=12_000_000, transcendentals=0
        ),
        name="prepare",
    )(tracers, wind_fields, low_t, high_t, low_w, high_w, perm, perm_w)

    advect = pl.pallas_call(
        functools.partial(advect_kernel, (inner, band_rows, per_level)),
        out_shape=jax.ShapeDtypeStruct((CAP * size, wide), BF16),
        in_specs=[vmem, anywhere, anywhere, anywhere],
        out_specs=vmem,
        scratch_shapes=[
            pltpu.VMEM((CAP, per_level, band_rows + 2 * RIM, padded_inner, LANES), F32),
            pltpu.VMEM((CAP, 2, band_rows + 2 * RIM, padded_inner, LANES), F32),
            pltpu.VMEM((wide, wide), BF16),
            pltpu.VMEM((CAP * size, wide), F32),
            pltpu.SMEM((CAP,), jnp.int32),
            pltpu.SemaphoreType.DMA((CAP, 2)),
            pltpu.SemaphoreType.DMA,
        ],
        cost_estimate=pl.CostEstimate(
            flops=16_000_000, bytes_accessed=6_000_000, transcendentals=0
        ),
        name="advect",
    )
    received = []
    for n in range(offsets):
        result = advect(arrived[n], fields, extra, perm)
        received.append(result if FIRST + n == 0 else shifted(result, "lon", FIRST + n))

    return pl.pallas_call(
        functools.partial(gather_kernel, (columns, rows, groups, inner, bands, band_rows)),
        out_shape=jax.ShapeDtypeStruct((columns, rows, tracer_ch), BF16),
        in_specs=[smem] + [vmem] * offsets,
        out_specs=vmem,
        scratch_shapes=[pltpu.VMEM((tracer_ch // LANES, columns * rows, LANES), F32)] + tables,
        cost_estimate=pl.CostEstimate(flops=2_000_000, bytes_accessed=6_000_000, transcendentals=0),
        name="gather",
    )(departures, *received)


def solution(mesh):
    placed = (
        P(("groups", "lon"), None, None),
        P(("groups", "lon"), None, None),
        P(("groups", "lon"), None, None),
    )
    return jax.shard_map(
        on_device,
        mesh=mesh,
        in_specs=placed,
        out_specs=P(("groups", "lon"), None, None),
        check_vma=False,
    )
```

```python
import functools

import jax
import jax.numpy as jnp
from jax import lax
from jax.experimental import pallas as pl
from jax.experimental.pallas import tpu as pltpu
from jax.sharding import PartitionSpec as P


CAP = 4
TRAJ = 3
FIRST = -4
LAST = 4
LATE = 3
ORDER = (2, -4, -2, 3, -3, 1, -1, 0)
RIM = 2
LANES = 128
META = 16
CLIP_BOUND = 0.95
F32 = jnp.float32
BF16 = jnp.bfloat16


def shifted(block, axis, distance):
    count = lax.axis_size(axis)
    route = [((i - distance) % count, i) for i in range(count)]
    return lax.ppermute(block, axis, route)


def fill_slots(dep_ref, slot_ref, count_ref, bands):
    for offset in range(LAST - FIRST):
        count_ref[offset] = 0
        for slot in range(CAP):
            slot_ref[offset * CAP + slot] = -1

    def place(band, carry):
        offset = dep_ref[0, 0, band] - FIRST
        ordinal = count_ref[offset]
        slot_ref[offset * CAP + ordinal] = band
        count_ref[offset] = ordinal + 1
        return carry

    lax.fori_loop(0, bands, place, 0)


def wind_perm(rows, levels, kinds):
    shape = (rows, kinds * LANES)
    row = lax.broadcasted_iota(jnp.int32, shape, 0)
    column = lax.broadcasted_iota(jnp.int32, shape, 1)
    bits = levels.bit_length() - 1
    kind = lax.shift_right_logical(row, bits) & 3
    group = lax.shift_right_logical(row, bits + 2)
    place = kind * LANES + group * levels + (row & (levels - 1))
    return jnp.where(place == column, 1.0, 0.0).astype(BF16)


def wind_kernel(sizes, dep_hbm_ref, wind_hbm_ref, tracers_ref, *rest):
    columns, rows, inner, bands, band_rows = sizes
    outs = rest[: LAST - FIRST]
    (
        dep_ref,
        wind_ref,
        wide_ref,
        here_ref,
        perm_ref,
        edge_ref,
        sem_ref,
        wind_sem_ref,
        slot_ref,
        count_ref,
    ) = rest[LAST - FIRST :]
    groups = columns // inner
    halves = tracers_ref.shape[-1] // LANES
    pitch = rows + 1
    chunks = [
        pltpu.make_async_copy(
            wind_hbm_ref.at[pl.ds(g * inner, inner)],
            wind_ref.at[pl.ds(g * inner, inner)],
            wind_sem_ref.at[g],
        )
        for g in range(groups)
    ]
    edges = [
        pltpu.make_async_copy(
            tracers_ref.at[pl.ds(side * (columns - RIM), RIM)], edge_ref.at[side], sem_ref.at[side]
        )
        for side in range(2)
    ]
    table = pltpu.make_async_copy(dep_hbm_ref, dep_ref, sem_ref.at[2])
    for copy in [table] + chunks + edges:
        copy.start()
    perm_ref[...] = wind_perm(perm_ref.shape[0], LANES // groups, 2)
    table.wait()
    fill_slots(dep_ref, slot_ref, count_ref, bands)

    def widen(column, carry):
        wide_ref[pl.ds(column * pitch, rows), :] = wind_ref[column].astype(F32)
        return carry

    for g in range(groups):
        chunks[g].wait()
        lax.fori_loop(g * inner, (g + 1) * inner, widen, 0, unroll=4)


    def some_rows(block, carry):
        left = jnp.concatenate(
            [
                jnp.concatenate(
                    [
                        wide_ref[pl.ds(g * inner * pitch + block * 16 + step, inner, stride=pitch), :]
                        for g in range(groups)
                    ],
                    axis=1,
                )
                for step in range(16)
            ],
            axis=0,
        ).astype(BF16)
        moved = jnp.dot(left, perm_ref[...], preferred_element_type=F32)
        for comp in range(2):
            here_ref[comp, pl.ds(block * 16, 16)] = moved[
                :, comp * LANES : (comp + 1) * LANES
            ].reshape(16, inner, LANES)
        return carry

    lax.fori_loop(0, rows // 16, some_rows, 0)
    lane = lax.broadcasted_iota(jnp.int32, (META, LANES), 1)
    size = band_rows * inner
    for offset in range(LAST - FIRST):
        meta = jnp.full((META, LANES), -1.0, F32)
        for slot in range(CAP):
            band = slot_ref[offset * CAP + slot]
            safe = jnp.maximum(band, 0)
            source = jnp.where(band >= 0, safe - dep_ref[0, 1, safe], -1)
            meta = jnp.where(lane == slot, source.astype(F32), meta)
            for comp in range(2):
                outs[offset][pl.ds((slot * 2 + comp) * size, size), :] = (
                    here_ref[comp, pl.ds(safe * band_rows, band_rows)]
                    .reshape(size, LANES)
                    .astype(BF16)
                )
        at = CAP * 2 * size
        outs[offset][pl.ds(at, META), :] = meta.astype(BF16)
        if abs(offset + FIRST) != 1:
            continue
        at += META
        side = 0 if offset + FIRST == 1 else 1
        edges[side].wait()
        for rim in range(RIM):
            column = side * (columns - RIM) + rim
            for half in range(halves):
                outs[offset][pl.ds(at, rows), :] = edge_ref[
                    side, rim, :, half * LANES : (half + 1) * LANES
                ]
                at += rows
            outs[offset][pl.ds(at, rows), :] = wind_ref[column]
            at += rows


def prepare_kernel(
    sizes,
    tracers_ref,
    wind_ref,
    low_ref,
    high_ref,
    perm_ref,
    out_t_ref,
    out_e_ref,
    wide_t_ref,
    wide_w_ref,
    wind_perm_ref,
):
    columns, rows, inner, padded_inner, rim_at = sizes
    batch = 16
    groups = columns // inner
    tracer_ch = tracers_ref.shape[-1]
    halves = tracer_ch // LANES
    pitch = rows + 1

    wind_perm_ref[...] = wind_perm(wind_perm_ref.shape[0], LANES // groups, 4)

    def own(column, carry):
        at = pl.ds((RIM + column) * pitch, rows)
        for half in range(halves):
            wide_t_ref[half, at, :] = tracers_ref[
                column, :, half * LANES : (half + 1) * LANES
            ].astype(F32)
        wide_w_ref[at, :] = wind_ref[column].astype(F32)
        return carry

    lax.fori_loop(0, columns, own, 0, unroll=4)
    for side, ref in ((0, low_ref), (columns + RIM, high_ref)):
        for rim in range(RIM):
            start = rim_at + rim * (halves + 1) * rows
            at = pl.ds((side + rim) * pitch, rows)
            for half in range(halves):
                wide_t_ref[half, at, :] = ref[pl.ds(start + half * rows, rows), :].astype(F32)
            wide_w_ref[at, :] = ref[pl.ds(start + halves * rows, rows), :].astype(F32)
    for column in range(columns + 2 * RIM, columns - inner + padded_inner):
        at = pl.ds(column * pitch, pitch)
        for half in range(halves):
            wide_t_ref[half, at, :] = jnp.zeros((pitch, LANES), F32)
        wide_w_ref[at, :] = jnp.zeros((pitch, LANES), F32)

    def some_rows(block, carry):
        parts_t = []
        parts_w = []
        for step in range(batch):
            pieces_t = []
            pieces_w = []
            for g in range(groups):
                at = pl.ds(g * inner * pitch + block * batch + step, padded_inner, stride=pitch)
                for half in range(halves):
                    pieces_t.append(wide_t_ref[half, at, :])
                pieces_w.append(wide_w_ref[at, :])
            parts_t.append(jnp.concatenate(pieces_t, axis=1))
            parts_w.append(jnp.concatenate(pieces_w, axis=1))
        left_t = jnp.concatenate(parts_t, axis=0).astype(BF16)
        left_w = jnp.concatenate(parts_w, axis=0).astype(BF16)
        at = pl.ds(RIM + block * batch, batch)
        shape = (batch, padded_inner, LANES)
        moved = jnp.dot(left_w, wind_perm_ref[...], preferred_element_type=F32)
        for comp in range(2):
            now = moved[:, comp * LANES : (comp + 1) * LANES]
            before = moved[:, (comp + 2) * LANES : (comp + 3) * LANES]
            out_e_ref[comp, at] = (2.0 * now - before).reshape(shape)
        moved = jnp.dot(left_t, perm_ref[...], preferred_element_type=F32)
        for kind in range(out_t_ref.shape[0]):
            out_t_ref[kind, at] = moved[:, kind * LANES : (kind + 1) * LANES].reshape(shape)
        return carry

    lax.fori_loop(0, rows // batch, some_rows, 0)
    for ref in (out_t_ref, out_e_ref):
        for kind in range(ref.shape[0]):
            for rim in range(RIM):
                ref[kind, rim] = ref[kind, RIM]
                ref[kind, RIM + rows + rim] = ref[kind, RIM + rows - 1]


def cubic_weights(shift):
    e = jnp.abs(shift)
    positive = shift > 0.0
    one_less = 1.0 - e
    one_more = 1.0 + e
    two_less = 2.0 - e
    center = 0.5 * one_less * two_less * one_more
    near = 0.5 * e * two_less * one_more
    across = e * one_less * (-1.0 / 6.0)
    beyond = across * two_less
    far = across * one_more
    zero = jnp.zeros_like(e)
    return (
        jnp.where(positive, far, zero),
        jnp.where(positive, near, beyond),
        center,
        jnp.where(positive, beyond, near),
        jnp.where(positive, zero, far),
    ), positive


def linear_weights(shift):
    return jnp.maximum(shift, 0.0), 1.0 - jnp.abs(shift), jnp.maximum(-shift, 0.0)


def clipped(value):
    return jnp.clip(value, -CLIP_BOUND, CLIP_BOUND)


def advect_kernel(sizes, msg_ref, t_ref, e_ref, perm_ref, out_ref, result_ref, source_ref):
    inner, band_rows = sizes
    size = band_rows * inner
    per_level = t_ref.shape[0]
    meta = msg_ref[pl.ds(CAP * 2 * size, META), :].astype(F32)
    lane = lax.broadcasted_iota(jnp.int32, (META, LANES), 1)
    for slot in range(CAP):
        source_ref[slot] = jnp.max(jnp.where(lane == slot, meta, -1.0)).astype(jnp.int32)

    def one_slot(slot, carry):
        source = source_ref[slot]

        @pl.when(source >= 0)
        def _():
            first = source * band_rows + RIM

            def one_row(row, inner_carry):
                here = [
                    msg_ref[pl.ds((slot * 2 + comp) * size + row * inner, inner), :].astype(F32)
                    for comp in range(2)
                ]
                for eight in range(inner // 8):
                    base = eight * 8
                    wind = [h[base : base + 8] for h in here]
                    window = [
                        [
                            [
                                e_ref[comp, first + row + b, pl.ds(base + RIM + a, 8), :]
                                for a in (-1, 0, 1)
                            ]
                            for b in (-1, 0, 1)
                        ]
                        for comp in range(2)
                    ]
                    shift = [clipped(w) for w in wind]
                    for _ in range(TRAJ):
                        lon = linear_weights(shift[0])
                        lat = linear_weights(shift[1])
                        moved = []
                        for comp in range(2):
                            total = None
                            for b in range(3):
                                line = (
                                    lon[0] * window[comp][b][0]
                                    + lon[1] * window[comp][b][1]
                                    + lon[2] * window[comp][b][2]
                                )
                                line = lat[b] * line
                                total = line if total is None else total + line
                            moved.append(clipped(0.5 * (wind[comp] + total)))
                        shift = moved
                    lon_cubic, _ = cubic_weights(shift[0])
                    lat_cubic, north = cubic_weights(shift[1])
                    low, mid, high = linear_weights(shift[0])
                    zero = jnp.zeros_like(low)
                    lon_linear = (zero, low, mid, high, zero)
                    taps = []
                    for b in range(-2, 3):
                        for a in range(-2, 3):
                            if abs(b) == 2:
                                if abs(a) == 2:
                                    continue
                                weight = lon_linear[a + 2]
                            elif b == 0:
                                weight = lon_cubic[a + 2]
                            elif b == -1:
                                weight = jnp.where(north, lon_cubic[a + 2], lon_linear[a + 2])
                            else:
                                weight = jnp.where(north, lon_linear[a + 2], lon_cubic[a + 2])
                            taps.append((a, b, weight * lat_cubic[b + 2]))
                    for tracer in range(per_level):
                        total = None
                        for a, b, weight in taps:
                            term = weight * t_ref[
                                tracer, first + row + b, pl.ds(base + RIM + a, 8), :
                            ]
                            total = term if total is None else total + term
                        result_ref[
                            pl.ds(slot * size + row * inner + base, 8),
                            tracer * LANES : (tracer + 1) * LANES,
                        ] = total
                return inner_carry

            lax.fori_loop(0, band_rows, one_row, 0)

        return carry

    lax.fori_loop(0, CAP, one_slot, 0)
    out_ref[...] = jnp.dot(
        result_ref[...].astype(BF16), perm_ref[...], preferred_element_type=F32
    ).astype(BF16)


def collect(sizes, slot_ref, ins, wide_ref):
    columns, rows, inner, _, band_rows = sizes
    pitch = rows + 1
    size = band_rows * inner
    halves = wide_ref.shape[0]
    for offset, in_ref in ins:

        def one_slot(slot, carry):
            band = slot_ref[(offset - FIRST) * CAP + slot]

            @pl.when(band >= 0)
            def _():
                for row in range(band_rows):
                    value = in_ref[pl.ds(slot * size + row * inner, inner), :]
                    for g in range(columns // inner):
                        at = pl.ds(
                            g * inner * pitch + band * band_rows + row, inner, stride=pitch
                        )
                        for half in range(halves):
                            first = (g * halves + half) * LANES
                            wide_ref[half, at, :] = value[:, first : first + LANES].astype(F32)

            return carry

        lax.fori_loop(0, CAP, one_slot, 0)


def early_kernel(sizes, offsets, dep_ref, *rest):
    ins = rest[: len(offsets)]
    wide_ref, slot_ref, count_ref = rest[len(offsets) :]
    fill_slots(dep_ref, slot_ref, count_ref, sizes[3])
    collect(sizes, slot_ref, zip(offsets, ins), wide_ref)


def late_kernel(sizes, offsets, dep_ref, *rest):
    columns, rows = sizes[:2]
    ins = rest[: len(offsets)]
    _, out_ref, wide_ref, slot_ref, count_ref, stage_ref, sem_ref = rest[len(offsets) :]
    fill_slots(dep_ref, slot_ref, count_ref, sizes[3])
    collect(sizes, slot_ref, zip(offsets, ins), wide_ref)
    pitch = rows + 1
    halves = wide_ref.shape[0]
    chunks = sem_ref.shape[0]
    width = columns // chunks
    copies = [
        pltpu.make_async_copy(
            stage_ref.at[pl.ds(n * width, width)], out_ref.at[pl.ds(n * width, width)], sem_ref.at[n]
        )
        for n in range(chunks)
    ]

    def narrow(column, carry):
        at = pl.ds(column * pitch, rows)
        for half in range(halves):
            stage_ref[column, :, half * LANES : (half + 1) * LANES] = wide_ref[half, at, :].astype(
                BF16
            )
        return carry

    for n in range(chunks):
        lax.fori_loop(n * width, (n + 1) * width, narrow, 0, unroll=4)
        copies[n].start()
    for copy in copies:
        copy.wait()


def on_device(tracers, wind_fields, departures):
    columns, rows, tracer_ch = tracers.shape
    levels = wind_fields.shape[-1] // 4
    per_level = tracer_ch // levels
    bands = departures.shape[1]
    band_rows = rows // bands
    inner = columns * levels // LANES
    padded_inner = -(-(inner + 2 * RIM) // 8) * 8
    size = band_rows * inner
    offsets = LAST - FIRST
    halves = tracer_ch // LANES
    rim_at = CAP * 2 * size + META
    rim_rows = RIM * (halves + 1) * rows

    wide = per_level * LANES
    index = jnp.arange(wide, dtype=jnp.int32)
    place = (index // levels) % (LANES // levels) * tracer_ch + index % levels * per_level
    place = place + index // LANES
    spread = (place[None, :] == index[:, None]).astype(BF16)
    join = (place[:, None] == index[None, :]).astype(BF16)
    table = jnp.transpose(departures, (0, 2, 1))

    vmem = pl.BlockSpec(memory_space=pltpu.VMEM)
    smem = pl.BlockSpec(memory_space=pltpu.SMEM)
    hbm = pl.BlockSpec(memory_space=pltpu.HBM)
    tables = [pltpu.SMEM((offsets * CAP,), jnp.int32), pltpu.SMEM((offsets,), jnp.int32)]

    def params(mib):
        return pltpu.CompilerParams(vmem_limit_bytes=mib << 20)

    messages = pl.pallas_call(
        functools.partial(wind_kernel, (columns, rows, inner, bands, band_rows)),
        out_shape=[
            jax.ShapeDtypeStruct((rim_at + (rim_rows if abs(n) == 1 else 0), LANES), BF16)
            for n in range(FIRST, LAST)
        ],
        in_specs=[hbm] * 3,
        out_specs=[vmem] * offsets,
        scratch_shapes=[
            pltpu.SMEM(table.shape, jnp.int32),
            pltpu.VMEM(wind_fields.shape, BF16),
            pltpu.VMEM((columns * (rows + 1), LANES), F32),
            pltpu.VMEM((2, rows, inner, LANES), F32),
            pltpu.VMEM((columns // inner * LANES, 2 * LANES), BF16),
            pltpu.VMEM((2, RIM, rows, tracer_ch), BF16),
            pltpu.SemaphoreType.DMA((3,)),
            pltpu.SemaphoreType.DMA((columns // inner,)),
        ]
        + tables,
        compiler_params=params(16),
        cost_estimate=pl.CostEstimate(flops=4_000_000, bytes_accessed=3_000_000, transcendentals=0),
        name="winds",
    )(*(pltpu.with_memory_space_constraint(x, pltpu.HBM) for x in (table, wind_fields, tracers)))

    arrived = {}
    for n in ORDER:
        msg = messages[n - FIRST]
        arrived[n] = msg if n == 0 else shifted(msg, "lon", -n)

    all_rows = (columns - inner + padded_inner) * (rows + 1)
    prepare = pl.pallas_call(
        functools.partial(prepare_kernel, (columns, rows, inner, padded_inner, rim_at)),
        out_shape=[
            jax.ShapeDtypeStruct((per_level, rows + 2 * RIM, padded_inner, LANES), F32),
            jax.ShapeDtypeStruct((2, rows + 2 * RIM, padded_inner, LANES), F32),
        ],
        in_specs=[vmem] * 5,
        out_specs=[vmem] * 2,
        scratch_shapes=[
            pltpu.VMEM((halves, all_rows, LANES), F32),
            pltpu.VMEM((all_rows, LANES), F32),
            pltpu.VMEM((columns // inner * LANES, 4 * LANES), BF16),
        ],
        compiler_params=params(32),
        cost_estimate=pl.CostEstimate(
            flops=16_000_000, bytes_accessed=12_000_000, transcendentals=0
        ),
        name="prepare",
    )
    fields, extra = prepare(tracers, wind_fields, arrived[-1], arrived[1], spread)

    advect = pl.pallas_call(
        functools.partial(advect_kernel, (inner, band_rows)),
        out_shape=jax.ShapeDtypeStruct((CAP * size, wide), BF16),
        in_specs=[vmem] * 4,
        out_specs=vmem,
        scratch_shapes=[
            pltpu.VMEM((CAP * size, wide), F32),
            pltpu.SMEM((CAP,), jnp.int32),
        ],
        compiler_params=params(12),
        cost_estimate=pl.CostEstimate(
            flops=16_000_000, bytes_accessed=6_000_000, transcendentals=0
        ),
        name="advect",
    )
    received = [None] * offsets
    for n in ORDER:
        result = advect(arrived[n], fields, extra, join)
        received[n - FIRST] = result if n == 0 else shifted(result, "lon", n)

    sizes = (columns, rows, inner, bands, band_rows)
    wide_shape = jax.ShapeDtypeStruct((halves, columns * (rows + 1), LANES), F32)
    early = ORDER[: offsets - 1 - LATE] + ORDER[-1:]
    late = ORDER[offsets - 1 - LATE : -1]
    first = pl.pallas_call(
        functools.partial(early_kernel, sizes, early),
        out_shape=wide_shape,
        in_specs=[smem] + [vmem] * len(early),
        out_specs=vmem,
        scratch_shapes=tables,
        compiler_params=params(8),
        cost_estimate=pl.CostEstimate(flops=2_000_000, bytes_accessed=6_000_000, transcendentals=0),
        name="early",
    )
    spread_out = first(table, *[received[n - FIRST] for n in early])
    last = pl.pallas_call(
        functools.partial(late_kernel, sizes, late),
        out_shape=[jax.ShapeDtypeStruct((columns, rows, tracer_ch), BF16), wide_shape],
        in_specs=[smem] + [vmem] * (len(late) + 1),
        out_specs=[pl.BlockSpec(memory_space=pl.ANY), vmem],
        scratch_shapes=tables
        + [pltpu.VMEM((columns, rows, tracer_ch), BF16), pltpu.SemaphoreType.DMA((8,))],
        input_output_aliases={len(late) + 1: 1},
        compiler_params=params(8),
        cost_estimate=pl.CostEstimate(flops=2_000_000, bytes_accessed=6_000_000, transcendentals=0),
        name="late",
    )
    return last(table, *[received[n - FIRST] for n in late], spread_out)[0]


def solution(mesh):
    placed = (
        P(("groups", "lon"), None, None),
        P(("groups", "lon"), None, None),
        P(("groups", "lon"), None, None),
    )
    return jax.shard_map(
        on_device,
        mesh=mesh,
        in_specs=placed,
        out_specs=P(("groups", "lon"), None, None),
        check_vma=False,
    )
```

```python
import functools

import jax
import jax.numpy as jnp
from jax import lax
from jax.experimental import pallas as pl
from jax.experimental.pallas import tpu as pltpu
from jax.sharding import PartitionSpec as P


CAP = 4
TRAJ = 3
FIRST = -4
LAST = 4
LATE = 3
ORDER = (-2, -4, 2, 3, -3, 1, -1, 0)
RIM = 2
LANES = 128
META = 16
CLIP_BOUND = 0.95
F32 = jnp.float32
BF16 = jnp.bfloat16


def shifted(block, axis, distance):
    count = lax.axis_size(axis)
    route = [((i - distance) % count, i) for i in range(count)]
    return lax.ppermute(block, axis, route)


def fill_slots(dep_ref, slot_ref, count_ref, bands):
    for offset in range(LAST - FIRST):
        count_ref[offset] = 0
        for slot in range(CAP):
            slot_ref[offset * CAP + slot] = -1

    def place(band, carry):
        offset = dep_ref[0, 0, band] - FIRST
        ordinal = count_ref[offset]
        slot_ref[offset * CAP + ordinal] = band
        count_ref[offset] = ordinal + 1
        return carry

    lax.fori_loop(0, bands, place, 0)


def wind_perm(rows, levels, kinds):
    shape = (rows, kinds * LANES)
    row = lax.broadcasted_iota(jnp.int32, shape, 0)
    column = lax.broadcasted_iota(jnp.int32, shape, 1)
    bits = levels.bit_length() - 1
    kind = lax.shift_right_logical(row, bits) & 3
    group = lax.shift_right_logical(row, bits + 2)
    place = kind * LANES + group * levels + (row & (levels - 1))
    return jnp.where(place == column, 1.0, 0.0).astype(BF16)


def tracer_perms(spread_ref, join_ref, groups, levels):
    per_level = join_ref.shape[0] // LANES
    tracer_ch = levels * per_level
    bits = per_level.bit_length() - 1

    def ones(place, offset):
        lane = lax.broadcasted_iota(jnp.int32, place.shape, 1)
        return jnp.where(place == lane - offset, 1.0, 0.0).astype(BF16)

    row = lax.broadcasted_iota(jnp.int32, (LANES, LANES), 0)
    group = lax.shift_right_logical(row, levels.bit_length() - 1)
    place = group * tracer_ch + (row & (levels - 1)) * per_level
    for tracer in range(per_level):
        for tile in range(per_level):
            join_ref[
                tracer * LANES : (tracer + 1) * LANES, tile * LANES : (tile + 1) * LANES
            ] = ones(place, tracer - tile * LANES)
    row = lax.broadcasted_iota(jnp.int32, (tracer_ch, LANES), 0)
    place = (row & (per_level - 1)) * LANES + lax.shift_right_logical(row, bits)
    for group in range(groups):
        for tile in range(per_level):
            spread_ref[
                group * tracer_ch : (group + 1) * tracer_ch, tile * LANES : (tile + 1) * LANES
            ] = ones(place, group * levels - tile * LANES)


def wind_kernel(sizes, dep_hbm_ref, wind_hbm_ref, tracers_ref, *rest):
    columns, rows, inner, bands, band_rows = sizes
    outs = rest[: LAST - FIRST]
    (
        spread_ref,
        join_ref,
        dep_ref,
        wind_ref,
        wide_ref,
        here_ref,
        perm_ref,
        edge_ref,
        sem_ref,
        wind_sem_ref,
        slot_ref,
        count_ref,
    ) = rest[LAST - FIRST :]
    groups = columns // inner
    halves = tracers_ref.shape[-1] // LANES
    pitch = rows + 1
    chunks = [
        pltpu.make_async_copy(
            wind_hbm_ref.at[pl.ds(g * inner, inner)],
            wind_ref.at[pl.ds(g * inner, inner)],
            wind_sem_ref.at[g],
        )
        for g in range(groups)
    ]
    edges = [
        pltpu.make_async_copy(
            tracers_ref.at[pl.ds(side * (columns - RIM), RIM)], edge_ref.at[side], sem_ref.at[side]
        )
        for side in range(2)
    ]
    table = pltpu.make_async_copy(dep_hbm_ref, dep_ref, sem_ref.at[2])
    for copy in [table] + chunks + edges:
        copy.start()
    perm_ref[...] = wind_perm(perm_ref.shape[0], LANES // groups, 2)
    tracer_perms(spread_ref, join_ref, groups, LANES // groups)
    table.wait()
    fill_slots(dep_ref, slot_ref, count_ref, bands)

    def widen(column, carry):
        wide_ref[pl.ds(column * pitch, rows), :] = wind_ref[column].astype(F32)
        return carry

    for g in range(groups):
        chunks[g].wait()
        lax.fori_loop(g * inner, (g + 1) * inner, widen, 0, unroll=4)


    def some_rows(block, carry):
        left = jnp.concatenate(
            [
                jnp.concatenate(
                    [
                        wide_ref[pl.ds(g * inner * pitch + block * 16 + step, inner, stride=pitch), :]
                        for g in range(groups)
                    ],
                    axis=1,
                )
                for step in range(16)
            ],
            axis=0,
        ).astype(BF16)
        moved = jnp.dot(left, perm_ref[...], preferred_element_type=F32)
        for comp in range(2):
            here_ref[comp, pl.ds(block * 16, 16)] = moved[
                :, comp * LANES : (comp + 1) * LANES
            ].reshape(16, inner, LANES)
        return carry

    lax.fori_loop(0, rows // 16, some_rows, 0)
    lane = lax.broadcasted_iota(jnp.int32, (META, LANES), 1)
    size = band_rows * inner
    for offset in range(LAST - FIRST):
        meta = jnp.full((META, LANES), -1.0, F32)
        for slot in range(CAP):
            band = slot_ref[offset * CAP + slot]
            safe = jnp.maximum(band, 0)
            source = jnp.where(band >= 0, safe - dep_ref[0, 1, safe], -1)
            meta = jnp.where(lane == slot, source.astype(F32), meta)
            for comp in range(2):
                outs[offset][pl.ds((slot * 2 + comp) * size, size), :] = (
                    here_ref[comp, pl.ds(safe * band_rows, band_rows)]
                    .reshape(size, LANES)
                    .astype(BF16)
                )
        at = CAP * 2 * size
        outs[offset][pl.ds(at, META), :] = meta.astype(BF16)
        if abs(offset + FIRST) != 1:
            continue
        at += META
        side = 0 if offset + FIRST == 1 else 1
        edges[side].wait()
        for rim in range(RIM):
            column = side * (columns - RIM) + rim
            for half in range(halves):
                outs[offset][pl.ds(at, rows), :] = edge_ref[
                    side, rim, :, half * LANES : (half + 1) * LANES
                ]
                at += rows
            outs[offset][pl.ds(at, rows), :] = wind_ref[column]
            at += rows


def prepare_kernel(
    sizes,
    tracers_ref,
    wind_ref,
    low_ref,
    high_ref,
    perm_ref,
    out_t_ref,
    out_e_ref,
    wide_t_ref,
    wide_w_ref,
    wind_perm_ref,
):
    columns, rows, inner, padded_inner, rim_at = sizes
    batch = 32
    groups = columns // inner
    tracer_ch = tracers_ref.shape[-1]
    halves = tracer_ch // LANES
    pitch = rows + 1

    wind_perm_ref[...] = wind_perm(wind_perm_ref.shape[0], LANES // groups, 4)

    def own(column, carry):
        at = pl.ds((RIM + column) * pitch, rows)
        for half in range(halves):
            wide_t_ref[half, at, :] = tracers_ref[
                column, :, half * LANES : (half + 1) * LANES
            ].astype(F32)
        wide_w_ref[at, :] = wind_ref[column].astype(F32)
        return carry

    lax.fori_loop(0, columns, own, 0, unroll=4)
    for side, ref in ((0, low_ref), (columns + RIM, high_ref)):
        for rim in range(RIM):
            start = rim_at + rim * (halves + 1) * rows
            at = pl.ds((side + rim) * pitch, rows)
            for half in range(halves):
                wide_t_ref[half, at, :] = ref[pl.ds(start + half * rows, rows), :].astype(F32)
            wide_w_ref[at, :] = ref[pl.ds(start + halves * rows, rows), :].astype(F32)
    for column in range(columns + 2 * RIM, columns - inner + padded_inner):
        at = pl.ds(column * pitch, pitch)
        for half in range(halves):
            wide_t_ref[half, at, :] = jnp.zeros((pitch, LANES), F32)
        wide_w_ref[at, :] = jnp.zeros((pitch, LANES), F32)

    def some_rows(block, carry):
        parts_t = []
        parts_w = []
        for step in range(batch):
            pieces_t = []
            pieces_w = []
            for g in range(groups):
                at = pl.ds(g * inner * pitch + block * batch + step, padded_inner, stride=pitch)
                for half in range(halves):
                    pieces_t.append(wide_t_ref[half, at, :])
                pieces_w.append(wide_w_ref[at, :])
            parts_t.append(jnp.concatenate(pieces_t, axis=1))
            parts_w.append(jnp.concatenate(pieces_w, axis=1))
        left_t = jnp.concatenate(parts_t, axis=0).astype(BF16)
        left_w = jnp.concatenate(parts_w, axis=0).astype(BF16)
        at = pl.ds(RIM + block * batch, batch)
        shape = (batch, padded_inner, LANES)
        moved = jnp.dot(left_w, wind_perm_ref[...], preferred_element_type=F32)
        for comp in range(2):
            now = moved[:, comp * LANES : (comp + 1) * LANES]
            before = moved[:, (comp + 2) * LANES : (comp + 3) * LANES]
            out_e_ref[comp, at] = (2.0 * now - before).reshape(shape)
        moved = jnp.dot(left_t, perm_ref[...], preferred_element_type=F32)
        for kind in range(out_t_ref.shape[0]):
            out_t_ref[kind, at] = moved[:, kind * LANES : (kind + 1) * LANES].reshape(shape)
        return carry

    lax.fori_loop(0, rows // batch, some_rows, 0)
    for ref in (out_t_ref, out_e_ref):
        for kind in range(ref.shape[0]):
            for rim in range(RIM):
                ref[kind, rim] = ref[kind, RIM]
                ref[kind, RIM + rows + rim] = ref[kind, RIM + rows - 1]


def cubic_weights(shift):
    e = jnp.abs(shift)
    positive = shift > 0.0
    one_less = 1.0 - e
    one_more = 1.0 + e
    two_less = 2.0 - e
    center = 0.5 * one_less * two_less * one_more
    near = 0.5 * e * two_less * one_more
    across = e * one_less * (-1.0 / 6.0)
    beyond = across * two_less
    far = across * one_more
    return (
        far,
        (jnp.where(positive, near, beyond), center, jnp.where(positive, beyond, near)),
        positive,
    )


def linear_weights(shift):
    return jnp.maximum(shift, 0.0), 1.0 - jnp.abs(shift), jnp.maximum(-shift, 0.0)


def clipped(value):
    return jnp.clip(value, -CLIP_BOUND, CLIP_BOUND)


def advect_kernel(sizes, msg_ref, t_ref, e_ref, perm_ref, out_ref, result_ref, source_ref):
    inner, band_rows = sizes
    size = band_rows * inner
    per_level = t_ref.shape[0]
    meta = msg_ref[pl.ds(CAP * 2 * size, META), :].astype(F32)
    lane = lax.broadcasted_iota(jnp.int32, (META, LANES), 1)
    for slot in range(CAP):
        source_ref[slot] = jnp.max(jnp.where(lane == slot, meta, -1.0)).astype(jnp.int32)

    def one_slot(slot, carry):
        source = source_ref[slot]

        @pl.when(source >= 0)
        def _():
            first = source * band_rows + RIM

            def one_row(row, inner_carry):
                here = [
                    msg_ref[pl.ds((slot * 2 + comp) * size + row * inner, inner), :].astype(F32)
                    for comp in range(2)
                ]
                for eight in range(inner // 8):
                    base = eight * 8
                    wind = [h[base : base + 8] for h in here]
                    window = [
                        [
                            [
                                e_ref[comp, first + row + b, pl.ds(base + RIM + a, 8), :]
                                for a in (-1, 0, 1)
                            ]
                            for b in (-1, 0, 1)
                        ]
                        for comp in range(2)
                    ]
                    shift = [clipped(w) for w in wind]
                    for _ in range(TRAJ):
                        lon = linear_weights(shift[0])
                        lat = linear_weights(shift[1])
                        moved = []
                        for comp in range(2):
                            total = None
                            for b in range(3):
                                line = (
                                    lon[0] * window[comp][b][0]
                                    + lon[1] * window[comp][b][1]
                                    + lon[2] * window[comp][b][2]
                                )
                                line = lat[b] * line
                                total = line if total is None else total + line
                            moved.append(clipped(0.5 * (wind[comp] + total)))
                        shift = moved
                    far, lon_cubic, east = cubic_weights(shift[0])
                    far_lat, lat_cubic, north = cubic_weights(shift[1])
                    low, mid, high = linear_weights(shift[0])
                    side = low + high
                    zero = jnp.zeros_like(low)
                    rows_of = []
                    for b, inside in ((-1, north), (0, None), (1, jnp.logical_not(north))):
                        weights = []
                        for cubic, linear in zip((far,) + lon_cubic, (zero, low, mid, high)):
                            if inside is not None:
                                cubic = jnp.where(inside, cubic, linear)
                            weights.append(cubic * lat_cubic[b + 1])
                        rows_of.append((b, weights))
                    mid = mid * far_lat
                    side = side * far_lat
                    for tracer in range(per_level):

                        def at(a, b):
                            return t_ref[tracer, first + row + b, pl.ds(base + RIM + a, 8), :]

                        edge = [jnp.where(north, at(a, -2), at(a, 2)) for a in (-1, 0, 1)]
                        total = mid * edge[1] + side * jnp.where(east, edge[0], edge[2])
                        for b, weights in rows_of:
                            total = total + weights[0] * jnp.where(east, at(-2, b), at(2, b))
                            for a in (-1, 0, 1):
                                total = total + weights[a + 2] * at(a, b)
                        result_ref[
                            pl.ds(slot * size + row * inner + base, 8),
                            tracer * LANES : (tracer + 1) * LANES,
                        ] = total
                return inner_carry

            lax.fori_loop(0, band_rows, one_row, 0)

        return carry

    lax.fori_loop(0, CAP, one_slot, 0)
    out_ref[...] = jnp.dot(
        result_ref[...].astype(BF16), perm_ref[...], preferred_element_type=F32
    ).astype(BF16)


def collect(sizes, slot_ref, ins, wide_ref):
    columns, rows, inner, _, band_rows = sizes
    pitch = rows + 1
    size = band_rows * inner
    halves = wide_ref.shape[0]
    for offset, in_ref in ins:

        def one_slot(slot, carry):
            band = slot_ref[(offset - FIRST) * CAP + slot]

            @pl.when(band >= 0)
            def _():
                for row in range(band_rows):
                    value = in_ref[pl.ds(slot * size + row * inner, inner), :]
                    for g in range(columns // inner):
                        at = pl.ds(
                            g * inner * pitch + band * band_rows + row, inner, stride=pitch
                        )
                        for half in range(halves):
                            first = (g * halves + half) * LANES
                            wide_ref[half, at, :] = value[:, first : first + LANES].astype(F32)

            return carry

        lax.fori_loop(0, CAP, one_slot, 0)


def early_kernel(sizes, offsets, dep_ref, *rest):
    ins = rest[: len(offsets)]
    wide_ref, slot_ref, count_ref = rest[len(offsets) :]
    fill_slots(dep_ref, slot_ref, count_ref, sizes[3])
    collect(sizes, slot_ref, zip(offsets, ins), wide_ref)


def late_kernel(sizes, offsets, dep_ref, *rest):
    columns, rows = sizes[:2]
    ins = rest[: len(offsets)]
    _, out_ref, wide_ref, slot_ref, count_ref, stage_ref, sem_ref = rest[len(offsets) :]
    fill_slots(dep_ref, slot_ref, count_ref, sizes[3])
    collect(sizes, slot_ref, zip(offsets, ins), wide_ref)
    pitch = rows + 1
    halves = wide_ref.shape[0]
    chunks = sem_ref.shape[0]
    width = columns // chunks
    copies = [
        pltpu.make_async_copy(
            stage_ref.at[pl.ds(n * width, width)], out_ref.at[pl.ds(n * width, width)], sem_ref.at[n]
        )
        for n in range(chunks)
    ]

    def narrow(column, carry):
        at = pl.ds(column * pitch, rows)
        for half in range(halves):
            stage_ref[column, :, half * LANES : (half + 1) * LANES] = wide_ref[half, at, :].astype(
                BF16
            )
        return carry

    for n in range(chunks):
        lax.fori_loop(n * width, (n + 1) * width, narrow, 0, unroll=4)
        copies[n].start()
    for copy in copies:
        copy.wait()


def on_device(tracers, wind_fields, departures):
    columns, rows, tracer_ch = tracers.shape
    levels = wind_fields.shape[-1] // 4
    per_level = tracer_ch // levels
    bands = departures.shape[1]
    band_rows = rows // bands
    inner = columns * levels // LANES
    padded_inner = -(-(inner + 2 * RIM) // 8) * 8
    size = band_rows * inner
    offsets = LAST - FIRST
    halves = tracer_ch // LANES
    rim_at = CAP * 2 * size + META
    rim_rows = RIM * (halves + 1) * rows

    wide = per_level * LANES
    table = jnp.transpose(departures, (0, 2, 1))

    vmem = pl.BlockSpec(memory_space=pltpu.VMEM)
    smem = pl.BlockSpec(memory_space=pltpu.SMEM)
    hbm = pl.BlockSpec(memory_space=pltpu.HBM)
    tables = [pltpu.SMEM((offsets * CAP,), jnp.int32), pltpu.SMEM((offsets,), jnp.int32)]

    def params(mib):
        return pltpu.CompilerParams(vmem_limit_bytes=mib << 20)

    *messages, spread, join = pl.pallas_call(
        functools.partial(wind_kernel, (columns, rows, inner, bands, band_rows)),
        out_shape=[
            jax.ShapeDtypeStruct((rim_at + (rim_rows if abs(n) == 1 else 0), LANES), BF16)
            for n in range(FIRST, LAST)
        ]
        + [jax.ShapeDtypeStruct((wide, wide), BF16)] * 2,
        in_specs=[hbm] * 3,
        out_specs=[vmem] * (offsets + 2),
        scratch_shapes=[
            pltpu.SMEM(table.shape, jnp.int32),
            pltpu.VMEM(wind_fields.shape, BF16),
            pltpu.VMEM((columns * (rows + 1), LANES), F32),
            pltpu.VMEM((2, rows, inner, LANES), F32),
            pltpu.VMEM((columns // inner * LANES, 2 * LANES), BF16),
            pltpu.VMEM((2, RIM, rows, tracer_ch), BF16),
            pltpu.SemaphoreType.DMA((3,)),
            pltpu.SemaphoreType.DMA((columns // inner,)),
        ]
        + tables,
        compiler_params=params(16),
        cost_estimate=pl.CostEstimate(flops=4_000_000, bytes_accessed=3_000_000, transcendentals=0),
        name="winds",
    )(*(pltpu.with_memory_space_constraint(x, pltpu.HBM) for x in (table, wind_fields, tracers)))

    arrived = {}
    for n in ORDER:
        msg = messages[n - FIRST]
        arrived[n] = msg if n == 0 else shifted(msg, "lon", -n)

    all_rows = (columns - inner + padded_inner) * (rows + 1)
    prepare = pl.pallas_call(
        functools.partial(prepare_kernel, (columns, rows, inner, padded_inner, rim_at)),
        out_shape=[
            jax.ShapeDtypeStruct((per_level, rows + 2 * RIM + 1, padded_inner, LANES), F32),
            jax.ShapeDtypeStruct((2, rows + 2 * RIM + 1, padded_inner, LANES), F32),
        ],
        in_specs=[vmem] * 5,
        out_specs=[vmem] * 2,
        scratch_shapes=[
            pltpu.VMEM((halves, all_rows, LANES), F32),
            pltpu.VMEM((all_rows, LANES), F32),
            pltpu.VMEM((columns // inner * LANES, 4 * LANES), BF16),
        ],
        compiler_params=params(32),
        cost_estimate=pl.CostEstimate(
            flops=16_000_000, bytes_accessed=12_000_000, transcendentals=0
        ),
        name="prepare",
    )
    fields, extra = prepare(tracers, wind_fields, arrived[-1], arrived[1], spread)

    advect = pl.pallas_call(
        functools.partial(advect_kernel, (inner, band_rows)),
        out_shape=jax.ShapeDtypeStruct((CAP * size, wide), BF16),
        in_specs=[vmem] * 4,
        out_specs=vmem,
        scratch_shapes=[
            pltpu.VMEM((CAP * size, wide), F32),
            pltpu.SMEM((CAP,), jnp.int32),
        ],
        compiler_params=params(12),
        cost_estimate=pl.CostEstimate(
            flops=16_000_000, bytes_accessed=6_000_000, transcendentals=0
        ),
        name="advect",
    )
    received = [None] * offsets
    for n in ORDER:
        result = advect(arrived[n], fields, extra, join)
        received[n - FIRST] = result if n == 0 else shifted(result, "lon", n)

    sizes = (columns, rows, inner, bands, band_rows)
    wide_shape = jax.ShapeDtypeStruct((halves, columns * (rows + 1), LANES), F32)
    early = ORDER[: offsets - 1 - LATE] + ORDER[-1:]
    late = ORDER[offsets - 1 - LATE : -1]
    first = pl.pallas_call(
        functools.partial(early_kernel, sizes, early),
        out_shape=wide_shape,
        in_specs=[smem] + [vmem] * len(early),
        out_specs=vmem,
        scratch_shapes=tables,
        compiler_params=params(8),
        cost_estimate=pl.CostEstimate(flops=2_000_000, bytes_accessed=6_000_000, transcendentals=0),
        name="early",
    )
    spread_out = first(table, *[received[n - FIRST] for n in early])
    last = pl.pallas_call(
        functools.partial(late_kernel, sizes, late),
        out_shape=[jax.ShapeDtypeStruct((columns, rows, tracer_ch), BF16), wide_shape],
        in_specs=[smem] + [vmem] * (len(late) + 1),
        out_specs=[pl.BlockSpec(memory_space=pl.ANY), vmem],
        scratch_shapes=tables
        + [pltpu.VMEM((columns, rows, tracer_ch), BF16), pltpu.SemaphoreType.DMA((8,))],
        input_output_aliases={len(late) + 1: 1},
        compiler_params=params(8),
        cost_estimate=pl.CostEstimate(flops=2_000_000, bytes_accessed=6_000_000, transcendentals=0),
        name="late",
    )
    return last(table, *[received[n - FIRST] for n in late], spread_out)[0]


def solution(mesh):
    placed = (
        P(("groups", "lon"), None, None),
        P(("groups", "lon"), None, None),
        P(("groups", "lon"), None, None),
    )
    return jax.shard_map(
        on_device,
        mesh=mesh,
        in_specs=placed,
        out_specs=P(("groups", "lon"), None, None),
        check_vma=False,
    )
```

```python
import functools

import jax
import jax.numpy as jnp
from jax import lax
from jax.experimental import pallas as pl
from jax.experimental.pallas import tpu as pltpu
from jax.sharding import PartitionSpec as P


CAP = 4
TRAJ = 3
FIRST = -4
LAST = 4
LATE = 3
ORDER = (-2, -4, 2, 3, -3, 1, -1, 0)
RIM = 2
LANES = 128
META = 8
CLIP_BOUND = 0.95
F32 = jnp.float32
BF16 = jnp.bfloat16


def shifted(block, axis, distance):
    count = lax.axis_size(axis)
    route = [((i - distance) % count, i) for i in range(count)]
    return lax.ppermute(block, axis, route)


def fill_slots(dep_ref, slot_ref, count_ref, bands):
    for offset in range(LAST - FIRST):
        count_ref[offset] = 0
        for slot in range(CAP):
            slot_ref[offset * CAP + slot] = -1

    def place(band, carry):
        offset = dep_ref[0, 0, band] - FIRST
        ordinal = count_ref[offset]
        slot_ref[offset * CAP + ordinal] = band
        count_ref[offset] = ordinal + 1
        return carry

    lax.fori_loop(0, bands, place, 0)


def wind_perm(rows, levels, kinds):
    shape = (rows, kinds * LANES)
    row = lax.broadcasted_iota(jnp.int32, shape, 0)
    column = lax.broadcasted_iota(jnp.int32, shape, 1)
    bits = levels.bit_length() - 1
    kind = lax.shift_right_logical(row, bits) & 3
    group = lax.shift_right_logical(row, bits + 2)
    place = kind * LANES + group * levels + (row & (levels - 1))
    return jnp.where(place == column, 1.0, 0.0).astype(BF16)


def tracer_perms(spread_ref, join_ref, groups, levels):
    per_level = join_ref.shape[0] // LANES
    tracer_ch = levels * per_level
    bits = per_level.bit_length() - 1

    def ones(place, offset):
        lane = lax.broadcasted_iota(jnp.int32, place.shape, 1)
        return jnp.where(place == lane - offset, 1.0, 0.0).astype(BF16)

    row = lax.broadcasted_iota(jnp.int32, (LANES, LANES), 0)
    group = lax.shift_right_logical(row, levels.bit_length() - 1)
    place = group * tracer_ch + (row & (levels - 1)) * per_level
    for tracer in range(per_level):
        for tile in range(per_level):
            join_ref[
                tracer * LANES : (tracer + 1) * LANES, tile * LANES : (tile + 1) * LANES
            ] = ones(place, tracer - tile * LANES)
    row = lax.broadcasted_iota(jnp.int32, (tracer_ch, LANES), 0)
    place = (row & (per_level - 1)) * LANES + lax.shift_right_logical(row, bits)
    for group in range(groups):
        for tile in range(per_level):
            spread_ref[
                group * tracer_ch : (group + 1) * tracer_ch, tile * LANES : (tile + 1) * LANES
            ] = ones(place, group * levels - tile * LANES)


def wind_kernel(sizes, dep_hbm_ref, wind_hbm_ref, tracers_ref, *rest):
    columns, rows, inner, bands, band_rows = sizes
    outs = rest[: LAST - FIRST]
    (
        spread_ref,
        join_ref,
        dep_ref,
        wind_ref,
        wide_ref,
        here_ref,
        perm_ref,
        edge_ref,
        sem_ref,
        wind_sem_ref,
        slot_ref,
        count_ref,
    ) = rest[LAST - FIRST :]
    groups = columns // inner
    halves = tracers_ref.shape[-1] // LANES
    pitch = rows + 1
    chunks = [
        pltpu.make_async_copy(
            wind_hbm_ref.at[pl.ds(g * inner, inner)],
            wind_ref.at[pl.ds(g * inner, inner)],
            wind_sem_ref.at[g],
        )
        for g in range(groups)
    ]
    edges = [
        pltpu.make_async_copy(
            tracers_ref.at[pl.ds(side * (columns - RIM), RIM)], edge_ref.at[side], sem_ref.at[side]
        )
        for side in range(2)
    ]
    table = pltpu.make_async_copy(dep_hbm_ref, dep_ref, sem_ref.at[2])
    for copy in [table] + chunks + edges:
        copy.start()
    perm_ref[...] = wind_perm(perm_ref.shape[0], LANES // groups, 2)
    tracer_perms(spread_ref, join_ref, groups, LANES // groups)
    table.wait()
    fill_slots(dep_ref, slot_ref, count_ref, bands)

    def widen(column, carry):
        wide_ref[pl.ds(column * pitch, rows), :] = wind_ref[column].astype(F32)
        return carry

    for g in range(groups):
        chunks[g].wait()
        lax.fori_loop(g * inner, (g + 1) * inner, widen, 0, unroll=4)


    def some_rows(block, carry):
        left = jnp.concatenate(
            [
                jnp.concatenate(
                    [
                        wide_ref[pl.ds(g * inner * pitch + block * 16 + step, inner, stride=pitch), :]
                        for g in range(groups)
                    ],
                    axis=1,
                )
                for step in range(16)
            ],
            axis=0,
        ).astype(BF16)
        moved = jnp.dot(left, perm_ref[...], preferred_element_type=F32)
        for comp in range(2):
            here_ref[comp, pl.ds(block * 16, 16)] = moved[
                :, comp * LANES : (comp + 1) * LANES
            ].reshape(16, inner, LANES)
        return carry

    lax.fori_loop(0, rows // 16, some_rows, 0)
    lane = lax.broadcasted_iota(jnp.int32, (META, LANES), 1)
    size = band_rows * inner
    for offset in range(LAST - FIRST):
        meta = jnp.full((META, LANES), -1.0, F32)
        for slot in range(CAP):
            band = slot_ref[offset * CAP + slot]
            safe = jnp.maximum(band, 0)
            source = jnp.where(band >= 0, safe - dep_ref[0, 1, safe], -1)
            meta = jnp.where(lane == slot, source.astype(F32), meta)
            for comp in range(2):
                outs[offset][pl.ds((slot * 2 + comp) * size, size), :] = (
                    here_ref[comp, pl.ds(safe * band_rows, band_rows)]
                    .reshape(size, LANES)
                    .astype(BF16)
                )
        at = CAP * 2 * size
        outs[offset][pl.ds(at, META), :] = meta.astype(BF16)
        if abs(offset + FIRST) != 1:
            continue
        at += META
        side = 0 if offset + FIRST == 1 else 1
        edges[side].wait()
        for rim in range(RIM):
            for half in range(halves):
                outs[offset][pl.ds(at, rows), :] = edge_ref[
                    side, rim, :, half * LANES : (half + 1) * LANES
                ]
                at += rows
        outs[offset][pl.ds(at, rows), :] = wind_ref[side * (columns - 1)]


def prepare_kernel(
    sizes,
    tracers_ref,
    wind_ref,
    low_ref,
    high_ref,
    perm_ref,
    out_t_ref,
    out_e_ref,
    wide_t_ref,
    wide_w_ref,
    wind_perm_ref,
):
    columns, rows, inner, padded_inner, rim_at = sizes
    batch = 32
    groups = columns // inner
    tracer_ch = tracers_ref.shape[-1]
    halves = tracer_ch // LANES
    pitch = rows + 1

    wind_perm_ref[...] = wind_perm(wind_perm_ref.shape[0], LANES // groups, 4)

    def own(column, carry):
        at = pl.ds((RIM + column) * pitch, rows)
        for half in range(halves):
            wide_t_ref[half, at, :] = tracers_ref[
                column, :, half * LANES : (half + 1) * LANES
            ].astype(F32)
        wide_w_ref[at, :] = wind_ref[column].astype(F32)
        return carry

    lax.fori_loop(0, columns, own, 0, unroll=4)
    for side, near, far, ref in (
        (0, RIM - 1, 0, low_ref),
        (columns + RIM, columns + RIM, columns + 2 * RIM - 1, high_ref),
    ):
        for rim in range(RIM):
            at = pl.ds((side + rim) * pitch, rows)
            for half in range(halves):
                wide_t_ref[half, at, :] = ref[
                    pl.ds(rim_at + (rim * halves + half) * rows, rows), :
                ].astype(F32)
        wide_w_ref[pl.ds(near * pitch, rows), :] = ref[
            pl.ds(rim_at + RIM * halves * rows, rows), :
        ].astype(F32)
        wide_w_ref[pl.ds(far * pitch, rows), :] = jnp.zeros((rows, LANES), F32)
    for column in range(columns + 2 * RIM, columns - inner + padded_inner):
        at = pl.ds(column * pitch, pitch)
        for half in range(halves):
            wide_t_ref[half, at, :] = jnp.zeros((pitch, LANES), F32)
        wide_w_ref[at, :] = jnp.zeros((pitch, LANES), F32)

    def some_rows(block, carry):
        parts_t = []
        parts_w = []
        for step in range(batch):
            pieces_t = []
            pieces_w = []
            for g in range(groups):
                at = pl.ds(g * inner * pitch + block * batch + step, padded_inner, stride=pitch)
                for half in range(halves):
                    pieces_t.append(wide_t_ref[half, at, :])
                pieces_w.append(wide_w_ref[at, :])
            parts_t.append(jnp.concatenate(pieces_t, axis=1))
            parts_w.append(jnp.concatenate(pieces_w, axis=1))
        left_t = jnp.concatenate(parts_t, axis=0).astype(BF16)
        left_w = jnp.concatenate(parts_w, axis=0).astype(BF16)
        at = pl.ds(RIM + block * batch, batch)
        shape = (batch, padded_inner, LANES)
        moved = jnp.dot(left_w, wind_perm_ref[...], preferred_element_type=F32)
        for comp in range(2):
            now = moved[:, comp * LANES : (comp + 1) * LANES]
            before = moved[:, (comp + 2) * LANES : (comp + 3) * LANES]
            out_e_ref[comp, at] = (2.0 * now - before).reshape(shape)
        moved = jnp.dot(left_t, perm_ref[...], preferred_element_type=F32)
        for kind in range(out_t_ref.shape[0]):
            out_t_ref[kind, at] = moved[:, kind * LANES : (kind + 1) * LANES].reshape(shape)
        return carry

    lax.fori_loop(0, rows // batch, some_rows, 0)
    for ref in (out_t_ref, out_e_ref):
        for kind in range(ref.shape[0]):
            for rim in range(RIM):
                ref[kind, rim] = ref[kind, RIM]
                ref[kind, RIM + rows + rim] = ref[kind, RIM + rows - 1]


def cubic_weights(shift):
    e = jnp.abs(shift)
    positive = shift > 0.0
    one_less = 1.0 - e
    one_more = 1.0 + e
    two_less = 2.0 - e
    center = 0.5 * one_less * two_less * one_more
    near = 0.5 * e * two_less * one_more
    across = e * one_less * (-1.0 / 6.0)
    beyond = across * two_less
    far = across * one_more
    return (
        far,
        (jnp.where(positive, near, beyond), center, jnp.where(positive, beyond, near)),
        positive,
    )


def linear_weights(shift):
    return jnp.maximum(shift, 0.0), 1.0 - jnp.abs(shift), jnp.maximum(-shift, 0.0)


def clipped(value):
    return jnp.clip(value, -CLIP_BOUND, CLIP_BOUND)


def advect_kernel(sizes, msg_ref, t_ref, e_ref, perm_ref, out_ref, result_ref, source_ref):
    inner, band_rows = sizes
    size = band_rows * inner
    per_level = t_ref.shape[0]
    meta = msg_ref[pl.ds(CAP * 2 * size, META), :].astype(F32)
    lane = lax.broadcasted_iota(jnp.int32, (META, LANES), 1)
    for slot in range(CAP):
        source_ref[slot] = jnp.max(jnp.where(lane == slot, meta, -1.0)).astype(jnp.int32)

    def one_slot(slot, carry):
        source = source_ref[slot]

        @pl.when(source >= 0)
        def _():
            first = source * band_rows + RIM

            def one_row(row, inner_carry):
                here = [
                    msg_ref[pl.ds((slot * 2 + comp) * size + row * inner, inner), :].astype(F32)
                    for comp in range(2)
                ]
                for eight in range(inner // 8):
                    base = eight * 8
                    wind = [h[base : base + 8] for h in here]
                    window = [
                        [
                            [
                                e_ref[comp, first + row + b, pl.ds(base + RIM + a, 8), :]
                                for a in (-1, 0, 1)
                            ]
                            for b in (-1, 0, 1)
                        ]
                        for comp in range(2)
                    ]
                    shift = [clipped(w) for w in wind]
                    for _ in range(TRAJ):
                        lon = linear_weights(shift[0])
                        lat = linear_weights(shift[1])
                        moved = []
                        for comp in range(2):
                            total = None
                            for b in range(3):
                                line = (
                                    lon[0] * window[comp][b][0]
                                    + lon[1] * window[comp][b][1]
                                    + lon[2] * window[comp][b][2]
                                )
                                line = lat[b] * line
                                total = line if total is None else total + line
                            moved.append(clipped(0.5 * (wind[comp] + total)))
                        shift = moved
                    far, lon_cubic, east = cubic_weights(shift[0])
                    far_lat, lat_cubic, north = cubic_weights(shift[1])
                    low, mid, high = linear_weights(shift[0])
                    side = low + high
                    zero = jnp.zeros_like(low)
                    rows_of = []
                    for b, inside in ((-1, north), (0, None), (1, jnp.logical_not(north))):
                        weights = []
                        for cubic, linear in zip((far,) + lon_cubic, (zero, low, mid, high)):
                            if inside is not None:
                                cubic = jnp.where(inside, cubic, linear)
                            weights.append(cubic * lat_cubic[b + 1])
                        rows_of.append((b, weights))
                    mid = mid * far_lat
                    side = side * far_lat
                    for tracer in range(per_level):

                        def at(a, b):
                            return t_ref[tracer, first + row + b, pl.ds(base + RIM + a, 8), :]

                        edge = [jnp.where(north, at(a, -2), at(a, 2)) for a in (-1, 0, 1)]
                        total = mid * edge[1] + side * jnp.where(east, edge[0], edge[2])
                        for b, weights in rows_of:
                            total = total + weights[0] * jnp.where(east, at(-2, b), at(2, b))
                            for a in (-1, 0, 1):
                                total = total + weights[a + 2] * at(a, b)
                        result_ref[
                            pl.ds(slot * size + row * inner + base, 8),
                            tracer * LANES : (tracer + 1) * LANES,
                        ] = total
                return inner_carry

            lax.fori_loop(0, band_rows, one_row, 0)

        return carry

    lax.fori_loop(0, CAP, one_slot, 0)
    out_ref[...] = jnp.dot(
        result_ref[...].astype(BF16), perm_ref[...], preferred_element_type=F32
    ).astype(BF16)


def collect(sizes, slot_ref, ins, wide_ref):
    columns, rows, inner, _, band_rows = sizes
    pitch = rows + 1
    size = band_rows * inner
    halves = wide_ref.shape[0]
    for offset, in_ref in ins:

        def one_slot(slot, carry):
            band = slot_ref[(offset - FIRST) * CAP + slot]

            @pl.when(band >= 0)
            def _():
                for row in range(band_rows):
                    value = in_ref[pl.ds(slot * size + row * inner, inner), :]
                    for g in range(columns // inner):
                        at = pl.ds(
                            g * inner * pitch + band * band_rows + row, inner, stride=pitch
                        )
                        for half in range(halves):
                            first = (g * halves + half) * LANES
                            wide_ref[half, at, :] = value[:, first : first + LANES].astype(F32)

            return carry

        lax.fori_loop(0, CAP, one_slot, 0)


def early_kernel(sizes, offsets, dep_ref, *rest):
    ins = rest[: len(offsets)]
    wide_ref, slot_ref, count_ref = rest[len(offsets) :]
    fill_slots(dep_ref, slot_ref, count_ref, sizes[3])
    collect(sizes, slot_ref, zip(offsets, ins), wide_ref)


def late_kernel(sizes, offsets, dep_ref, *rest):
    columns, rows = sizes[:2]
    ins = rest[: len(offsets)]
    _, out_ref, wide_ref, slot_ref, count_ref, stage_ref, sem_ref = rest[len(offsets) :]
    fill_slots(dep_ref, slot_ref, count_ref, sizes[3])
    collect(sizes, slot_ref, zip(offsets, ins), wide_ref)
    pitch = rows + 1
    halves = wide_ref.shape[0]
    chunks = sem_ref.shape[0]
    width = columns // chunks
    copies = [
        pltpu.make_async_copy(
            stage_ref.at[pl.ds(n * width, width)], out_ref.at[pl.ds(n * width, width)], sem_ref.at[n]
        )
        for n in range(chunks)
    ]

    def narrow(column, carry):
        at = pl.ds(column * pitch, rows)
        for half in range(halves):
            stage_ref[column, :, half * LANES : (half + 1) * LANES] = wide_ref[half, at, :].astype(
                BF16
            )
        return carry

    for n in range(chunks):
        lax.fori_loop(n * width, (n + 1) * width, narrow, 0, unroll=4)
        copies[n].start()
    for copy in copies:
        copy.wait()


def on_device(tracers, wind_fields, departures):
    columns, rows, tracer_ch = tracers.shape
    levels = wind_fields.shape[-1] // 4
    per_level = tracer_ch // levels
    bands = departures.shape[1]
    band_rows = rows // bands
    inner = columns * levels // LANES
    padded_inner = -(-(inner + 2 * RIM) // 8) * 8
    size = band_rows * inner
    offsets = LAST - FIRST
    halves = tracer_ch // LANES
    rim_at = CAP * 2 * size + META
    rim_rows = (RIM * halves + 1) * rows

    wide = per_level * LANES
    table = jnp.transpose(departures, (0, 2, 1))

    vmem = pl.BlockSpec(memory_space=pltpu.VMEM)
    smem = pl.BlockSpec(memory_space=pltpu.SMEM)
    hbm = pl.BlockSpec(memory_space=pltpu.HBM)
    tables = [pltpu.SMEM((offsets * CAP,), jnp.int32), pltpu.SMEM((offsets,), jnp.int32)]

    def params(mib):
        return pltpu.CompilerParams(vmem_limit_bytes=mib << 20)

    *messages, spread, join = pl.pallas_call(
        functools.partial(wind_kernel, (columns, rows, inner, bands, band_rows)),
        out_shape=[
            jax.ShapeDtypeStruct((rim_at + (rim_rows if abs(n) == 1 else 0), LANES), BF16)
            for n in range(FIRST, LAST)
        ]
        + [jax.ShapeDtypeStruct((wide, wide), BF16)] * 2,
        in_specs=[hbm] * 3,
        out_specs=[vmem] * (offsets + 2),
        scratch_shapes=[
            pltpu.SMEM(table.shape, jnp.int32),
            pltpu.VMEM(wind_fields.shape, BF16),
            pltpu.VMEM((columns * (rows + 1), LANES), F32),
            pltpu.VMEM((2, rows, inner, LANES), F32),
            pltpu.VMEM((columns // inner * LANES, 2 * LANES), BF16),
            pltpu.VMEM((2, RIM, rows, tracer_ch), BF16),
            pltpu.SemaphoreType.DMA((3,)),
            pltpu.SemaphoreType.DMA((columns // inner,)),
        ]
        + tables,
        compiler_params=params(16),
        cost_estimate=pl.CostEstimate(flops=4_000_000, bytes_accessed=3_000_000, transcendentals=0),
        name="winds",
    )(*(pltpu.with_memory_space_constraint(x, pltpu.HBM) for x in (table, wind_fields, tracers)))

    arrived = {}
    for n in ORDER:
        msg = messages[n - FIRST]
        arrived[n] = msg if n == 0 else shifted(msg, "lon", -n)

    all_rows = (columns - inner + padded_inner) * (rows + 1)
    prepare = pl.pallas_call(
        functools.partial(prepare_kernel, (columns, rows, inner, padded_inner, rim_at)),
        out_shape=[
            jax.ShapeDtypeStruct((per_level, rows + 2 * RIM + 1, padded_inner, LANES), F32),
            jax.ShapeDtypeStruct((2, rows + 2 * RIM + 1, padded_inner, LANES), F32),
        ],
        in_specs=[vmem] * 5,
        out_specs=[vmem] * 2,
        scratch_shapes=[
            pltpu.VMEM((halves, all_rows, LANES), F32),
            pltpu.VMEM((all_rows, LANES), F32),
            pltpu.VMEM((columns // inner * LANES, 4 * LANES), BF16),
        ],
        compiler_params=params(32),
        cost_estimate=pl.CostEstimate(
            flops=16_000_000, bytes_accessed=12_000_000, transcendentals=0
        ),
        name="prepare",
    )
    fields, extra = prepare(tracers, wind_fields, arrived[-1], arrived[1], spread)

    advect = pl.pallas_call(
        functools.partial(advect_kernel, (inner, band_rows)),
        out_shape=jax.ShapeDtypeStruct((CAP * size, wide), BF16),
        in_specs=[vmem] * 4,
        out_specs=vmem,
        scratch_shapes=[
            pltpu.VMEM((CAP * size, wide), F32),
            pltpu.SMEM((CAP,), jnp.int32),
        ],
        compiler_params=params(12),
        cost_estimate=pl.CostEstimate(
            flops=16_000_000, bytes_accessed=6_000_000, transcendentals=0
        ),
        name="advect",
    )
    received = [None] * offsets
    for n in ORDER:
        result = advect(arrived[n], fields, extra, join)
        received[n - FIRST] = result if n == 0 else shifted(result, "lon", n)

    sizes = (columns, rows, inner, bands, band_rows)
    wide_shape = jax.ShapeDtypeStruct((halves, columns * (rows + 1), LANES), F32)
    early = ORDER[: offsets - 1 - LATE] + ORDER[-1:]
    late = ORDER[offsets - 1 - LATE : -1]
    first = pl.pallas_call(
        functools.partial(early_kernel, sizes, early),
        out_shape=wide_shape,
        in_specs=[smem] + [vmem] * len(early),
        out_specs=vmem,
        scratch_shapes=tables,
        compiler_params=params(8),
        cost_estimate=pl.CostEstimate(flops=2_000_000, bytes_accessed=6_000_000, transcendentals=0),
        name="early",
    )
    spread_out = first(table, *[received[n - FIRST] for n in early])
    last = pl.pallas_call(
        functools.partial(late_kernel, sizes, late),
        out_shape=[jax.ShapeDtypeStruct((columns, rows, tracer_ch), BF16), wide_shape],
        in_specs=[smem] + [vmem] * (len(late) + 1),
        out_specs=[pl.BlockSpec(memory_space=pl.ANY), vmem],
        scratch_shapes=tables
        + [pltpu.VMEM((columns, rows, tracer_ch), BF16), pltpu.SemaphoreType.DMA((8,))],
        input_output_aliases={len(late) + 1: 1},
        compiler_params=params(8),
        cost_estimate=pl.CostEstimate(flops=2_000_000, bytes_accessed=6_000_000, transcendentals=0),
        name="late",
    )
    return last(table, *[received[n - FIRST] for n in late], spread_out)[0]


def solution(mesh):
    placed = (
        P(("groups", "lon"), None, None),
        P(("groups", "lon"), None, None),
        P(("groups", "lon"), None, None),
    )
    return jax.shard_map(
        on_device,
        mesh=mesh,
        in_specs=placed,
        out_specs=P(("groups", "lon"), None, None),
        check_vma=False,
    )
```

```python
import functools

import jax
import jax.numpy as jnp
from jax import lax
from jax.experimental import pallas as pl
from jax.experimental.pallas import tpu as pltpu
from jax.sharding import PartitionSpec as P


CAP = 4
TRAJ = 3
FIRST = -4
LAST = 4
LATE = 3
ORDER = (-2, -4, 2, 3, -3, 1, -1, 0)
RIM = 2
LANES = 128
META = 8
CLIP_BOUND = 0.95
F32 = jnp.float32
BF16 = jnp.bfloat16


def shifted(block, axis, distance):
    count = lax.axis_size(axis)
    route = [((i - distance) % count, i) for i in range(count)]
    return lax.ppermute(block, axis, route)


def fill_slots(dep_ref, slot_ref, count_ref, bands):
    for offset in range(LAST - FIRST):
        count_ref[offset] = 0
        for slot in range(CAP):
            slot_ref[offset * CAP + slot] = -1

    def place(band, carry):
        offset = dep_ref[0, 0, band] - FIRST
        ordinal = count_ref[offset]
        slot_ref[offset * CAP + ordinal] = band
        count_ref[offset] = ordinal + 1
        return carry

    lax.fori_loop(0, bands, place, 0)


def wind_perm(rows, levels, kinds):
    shape = (rows, kinds * LANES)
    row = lax.broadcasted_iota(jnp.int32, shape, 0)
    column = lax.broadcasted_iota(jnp.int32, shape, 1)
    bits = levels.bit_length() - 1
    kind = lax.shift_right_logical(row, bits) & 3
    group = lax.shift_right_logical(row, bits + 2)
    place = kind * LANES + group * levels + (row & (levels - 1))
    return jnp.where(place == column, 1.0, 0.0).astype(BF16)


def tracer_perms(spread_ref, join_ref, groups, levels):
    per_level = join_ref.shape[0] // LANES
    tracer_ch = levels * per_level
    bits = per_level.bit_length() - 1

    def ones(place, offset):
        lane = lax.broadcasted_iota(jnp.int32, place.shape, 1)
        return jnp.where(place == lane - offset, 1.0, 0.0).astype(BF16)

    row = lax.broadcasted_iota(jnp.int32, (LANES, LANES), 0)
    group = lax.shift_right_logical(row, levels.bit_length() - 1)
    place = group * tracer_ch + (row & (levels - 1)) * per_level
    for tracer in range(per_level):
        for tile in range(per_level):
            join_ref[
                tracer * LANES : (tracer + 1) * LANES, tile * LANES : (tile + 1) * LANES
            ] = ones(place, tracer - tile * LANES)
    row = lax.broadcasted_iota(jnp.int32, (tracer_ch, LANES), 0)
    place = (row & (per_level - 1)) * LANES + lax.shift_right_logical(row, bits)
    for group in range(groups):
        for tile in range(per_level):
            spread_ref[
                group * tracer_ch : (group + 1) * tracer_ch, tile * LANES : (tile + 1) * LANES
            ] = ones(place, group * levels - tile * LANES)


def wind_kernel(sizes, dep_hbm_ref, wind_hbm_ref, tracers_ref, *rest):
    columns, rows, inner, bands, band_rows = sizes
    outs = rest[: LAST - FIRST]
    (
        spread_ref,
        join_ref,
        dep_ref,
        wind_ref,
        wide_ref,
        here_ref,
        perm_ref,
        edge_ref,
        sem_ref,
        wind_sem_ref,
        slot_ref,
        count_ref,
    ) = rest[LAST - FIRST :]
    groups = columns // inner
    halves = tracers_ref.shape[-1] // LANES
    pitch = rows + 1
    chunks = [
        pltpu.make_async_copy(
            wind_hbm_ref.at[pl.ds(g * inner, inner)],
            wind_ref.at[pl.ds(g * inner, inner)],
            wind_sem_ref.at[g],
        )
        for g in range(groups)
    ]
    edges = [
        pltpu.make_async_copy(
            tracers_ref.at[pl.ds(side * (columns - RIM), RIM)], edge_ref.at[side], sem_ref.at[side]
        )
        for side in range(2)
    ]
    table = pltpu.make_async_copy(dep_hbm_ref, dep_ref, sem_ref.at[2])
    for copy in [table] + chunks + edges:
        copy.start()
    perm_ref[...] = wind_perm(perm_ref.shape[0], LANES // groups, 2)
    tracer_perms(spread_ref, join_ref, groups, LANES // groups)
    table.wait()
    fill_slots(dep_ref, slot_ref, count_ref, bands)

    def widen(column, carry):
        wide_ref[pl.ds(column * pitch, rows), :] = wind_ref[column].astype(F32)
        return carry

    for g in range(groups):
        chunks[g].wait()
        lax.fori_loop(g * inner, (g + 1) * inner, widen, 0, unroll=4)


    def some_rows(block, carry):
        left = jnp.concatenate(
            [
                jnp.concatenate(
                    [
                        wide_ref[pl.ds(g * inner * pitch + block * 16 + step, inner, stride=pitch), :]
                        for g in range(groups)
                    ],
                    axis=1,
                )
                for step in range(16)
            ],
            axis=0,
        ).astype(BF16)
        moved = jnp.dot(left, perm_ref[...], preferred_element_type=F32)
        for comp in range(2):
            here_ref[comp, pl.ds(block * 16, 16)] = moved[
                :, comp * LANES : (comp + 1) * LANES
            ].reshape(16, inner, LANES)
        return carry

    lax.fori_loop(0, rows // 16, some_rows, 0)
    lane = lax.broadcasted_iota(jnp.int32, (META, LANES), 1)
    size = band_rows * inner
    for offset in range(LAST - FIRST):
        meta = jnp.full((META, LANES), -1.0, F32)
        for slot in range(CAP):
            band = slot_ref[offset * CAP + slot]
            safe = jnp.maximum(band, 0)
            source = jnp.where(band >= 0, safe - dep_ref[0, 1, safe], -1)
            meta = jnp.where(lane == slot, source.astype(F32), meta)
            for comp in range(2):
                outs[offset][pl.ds((slot * 2 + comp) * size, size), :] = (
                    here_ref[comp, pl.ds(safe * band_rows, band_rows)]
                    .reshape(size, LANES)
                    .astype(BF16)
                )
        at = CAP * 2 * size
        outs[offset][pl.ds(at, META), :] = meta.astype(BF16)
        if abs(offset + FIRST) != 1:
            continue
        at += META
        side = 0 if offset + FIRST == 1 else 1
        edges[side].wait()
        for rim in range(RIM):
            for half in range(halves):
                outs[offset][pl.ds(at, rows), :] = edge_ref[
                    side, rim, :, half * LANES : (half + 1) * LANES
                ]
                at += rows
        outs[offset][pl.ds(at, rows), :] = wind_ref[side * (columns - 1)]


def prepare_kernel(
    sizes,
    tracers_ref,
    wind_ref,
    low_ref,
    high_ref,
    perm_ref,
    out_t_ref,
    out_e_ref,
    wide_t_ref,
    wide_w_ref,
    wind_perm_ref,
):
    columns, rows, inner, padded_inner, rim_at = sizes
    batch = 32
    groups = columns // inner
    tracer_ch = tracers_ref.shape[-1]
    halves = tracer_ch // LANES
    pitch = rows + 1

    wind_perm_ref[...] = wind_perm(wind_perm_ref.shape[0], LANES // groups, 4)

    def own(column, carry):
        at = pl.ds((RIM + column) * pitch, rows)
        for half in range(halves):
            wide_t_ref[half, at, :] = tracers_ref[
                column, :, half * LANES : (half + 1) * LANES
            ].astype(F32)
        wide_w_ref[at, :] = wind_ref[column].astype(F32)
        return carry

    lax.fori_loop(0, columns, own, 0, unroll=4)
    for side, near, far, ref in (
        (0, RIM - 1, 0, low_ref),
        (columns + RIM, columns + RIM, columns + 2 * RIM - 1, high_ref),
    ):
        for rim in range(RIM):
            at = pl.ds((side + rim) * pitch, rows)
            for half in range(halves):
                wide_t_ref[half, at, :] = ref[
                    pl.ds(rim_at + (rim * halves + half) * rows, rows), :
                ].astype(F32)
        wide_w_ref[pl.ds(near * pitch, rows), :] = ref[
            pl.ds(rim_at + RIM * halves * rows, rows), :
        ].astype(F32)
        wide_w_ref[pl.ds(far * pitch, rows), :] = jnp.zeros((rows, LANES), F32)
    for column in range(columns + 2 * RIM, columns - inner + padded_inner):
        at = pl.ds(column * pitch, pitch)
        for half in range(halves):
            wide_t_ref[half, at, :] = jnp.zeros((pitch, LANES), F32)
        wide_w_ref[at, :] = jnp.zeros((pitch, LANES), F32)

    def some_rows(block, carry):
        parts_t = []
        parts_w = []
        for step in range(batch):
            pieces_t = []
            pieces_w = []
            for g in range(groups):
                at = pl.ds(g * inner * pitch + block * batch + step, padded_inner, stride=pitch)
                for half in range(halves):
                    pieces_t.append(wide_t_ref[half, at, :])
                pieces_w.append(wide_w_ref[at, :])
            parts_t.append(jnp.concatenate(pieces_t, axis=1))
            parts_w.append(jnp.concatenate(pieces_w, axis=1))
        left_t = jnp.concatenate(parts_t, axis=0).astype(BF16)
        left_w = jnp.concatenate(parts_w, axis=0).astype(BF16)
        at = pl.ds(RIM + block * batch, batch)
        shape = (batch, padded_inner, LANES)
        moved = jnp.dot(left_w, wind_perm_ref[...], preferred_element_type=F32)
        for comp in range(2):
            now = moved[:, comp * LANES : (comp + 1) * LANES]
            before = moved[:, (comp + 2) * LANES : (comp + 3) * LANES]
            out_e_ref[comp, at] = (2.0 * now - before).reshape(shape)
        moved = jnp.dot(left_t, perm_ref[...], preferred_element_type=F32)
        for kind in range(out_t_ref.shape[0]):
            out_t_ref[kind, at] = moved[:, kind * LANES : (kind + 1) * LANES].reshape(shape)
        return carry

    lax.fori_loop(0, rows // batch, some_rows, 0)
    for ref in (out_t_ref, out_e_ref):
        for kind in range(ref.shape[0]):
            for rim in range(RIM):
                ref[kind, rim] = ref[kind, RIM]
                ref[kind, RIM + rows + rim] = ref[kind, RIM + rows - 1]


def cubic_weights(shift):
    e = jnp.abs(shift)
    positive = shift > 0.0
    one_less = 1.0 - e
    one_more = 1.0 + e
    two_less = 2.0 - e
    center = 0.5 * one_less * two_less * one_more
    near = 0.5 * e * two_less * one_more
    across = e * one_less * (-1.0 / 6.0)
    beyond = across * two_less
    far = across * one_more
    return (
        far,
        (jnp.where(positive, near, beyond), center, jnp.where(positive, beyond, near)),
        positive,
    )


def linear_weights(shift):
    return jnp.maximum(shift, 0.0), 1.0 - jnp.abs(shift), jnp.maximum(-shift, 0.0)


def clipped(value):
    return jnp.clip(value, -CLIP_BOUND, CLIP_BOUND)


def advect_kernel(sizes, msg_ref, t_ref, e_ref, perm_ref, out_ref, result_ref, source_ref):
    inner, band_rows = sizes
    size = band_rows * inner
    per_level = t_ref.shape[0]
    meta = msg_ref[pl.ds(CAP * 2 * size, META), :].astype(F32)
    lane = lax.broadcasted_iota(jnp.int32, (META, LANES), 1)
    for slot in range(CAP):
        source_ref[slot] = jnp.max(jnp.where(lane == slot, meta, -1.0)).astype(jnp.int32)

    def one_slot(slot, carry):
        source = source_ref[slot]

        @pl.when(source >= 0)
        def _():
            first = source * band_rows + RIM

            def one_row(row, inner_carry):
                here = [
                    msg_ref[pl.ds((slot * 2 + comp) * size + row * inner, inner), :].astype(F32)
                    for comp in range(2)
                ]
                for eight in range(inner // 8):
                    base = eight * 8
                    wind = [h[base : base + 8] for h in here]
                    window = [
                        [
                            [
                                e_ref[comp, first + row + b, pl.ds(base + RIM + a, 8), :]
                                for a in (-1, 0, 1)
                            ]
                            for b in (-1, 0, 1)
                        ]
                        for comp in range(2)
                    ]
                    shift = [clipped(w) for w in wind]
                    for _ in range(TRAJ):
                        lon = linear_weights(shift[0])
                        lat = linear_weights(shift[1])
                        moved = []
                        for comp in range(2):
                            total = None
                            for b in range(3):
                                line = (
                                    lon[0] * window[comp][b][0]
                                    + lon[1] * window[comp][b][1]
                                    + lon[2] * window[comp][b][2]
                                )
                                line = lat[b] * line
                                total = line if total is None else total + line
                            moved.append(clipped(0.5 * (wind[comp] + total)))
                        shift = moved
                    far, lon_cubic, east = cubic_weights(shift[0])
                    far_lat, lat_cubic, north = cubic_weights(shift[1])
                    low, mid, high = linear_weights(shift[0])
                    side = low + high
                    zero = jnp.zeros_like(low)
                    rows_of = []
                    for b, inside in ((-1, north), (0, None), (1, jnp.logical_not(north))):
                        weights = []
                        for cubic, linear in zip((far,) + lon_cubic, (zero, low, mid, high)):
                            if inside is not None:
                                cubic = jnp.where(inside, cubic, linear)
                            weights.append(cubic * lat_cubic[b + 1])
                        rows_of.append((b, weights))
                    mid = mid * far_lat
                    side = side * far_lat
                    for tracer in range(per_level):

                        def at(a, b):
                            return t_ref[tracer, first + row + b, pl.ds(base + RIM + a, 8), :]

                        edge = [jnp.where(north, at(a, -2), at(a, 2)) for a in (-1, 0, 1)]
                        total = mid * edge[1] + side * jnp.where(east, edge[0], edge[2])
                        for b, weights in rows_of:
                            total = total + weights[0] * jnp.where(east, at(-2, b), at(2, b))
                            for a in (-1, 0, 1):
                                total = total + weights[a + 2] * at(a, b)
                        result_ref[
                            pl.ds(slot * size + row * inner + base, 8),
                            tracer * LANES : (tracer + 1) * LANES,
                        ] = total
                return inner_carry

            lax.fori_loop(0, band_rows, one_row, 0)

        return carry

    lax.fori_loop(0, CAP, one_slot, 0)
    out_ref[...] = jnp.dot(
        result_ref[...].astype(BF16), perm_ref[...], preferred_element_type=F32
    ).astype(BF16)


def collect(sizes, slot_ref, ins, wide_ref):
    columns, rows, inner, _, band_rows = sizes
    pitch = rows + 1
    size = band_rows * inner
    halves = wide_ref.shape[0]
    for offset, in_ref in ins:

        def one_slot(slot, carry):
            band = slot_ref[(offset - FIRST) * CAP + slot]

            @pl.when(band >= 0)
            def _():
                for row in range(band_rows):
                    value = in_ref[pl.ds(slot * size + row * inner, inner), :]
                    for g in range(columns // inner):
                        at = pl.ds(
                            g * inner * pitch + band * band_rows + row, inner, stride=pitch
                        )
                        for half in range(halves):
                            first = (g * halves + half) * LANES
                            wide_ref[half, at, :] = value[:, first : first + LANES].astype(F32)

            return carry

        lax.fori_loop(0, CAP, one_slot, 0)


def early_kernel(sizes, offsets, dep_ref, *rest):
    ins = rest[: len(offsets)]
    wide_ref, slot_ref, count_ref = rest[len(offsets) :]
    fill_slots(dep_ref, slot_ref, count_ref, sizes[3])
    collect(sizes, slot_ref, zip(offsets, ins), wide_ref)


def late_kernel(sizes, offsets, slot_ref, *rest):
    columns, rows = sizes[:2]
    ins = rest[: len(offsets)]
    _, out_ref, wide_ref, stage_ref, sem_ref = rest[len(offsets) :]
    collect(sizes, slot_ref, zip(offsets, ins), wide_ref)
    pitch = rows + 1
    halves = wide_ref.shape[0]
    chunks = sem_ref.shape[0]
    width = columns // chunks
    copies = [
        pltpu.make_async_copy(
            stage_ref.at[pl.ds(n * width, width)], out_ref.at[pl.ds(n * width, width)], sem_ref.at[n]
        )
        for n in range(chunks)
    ]

    def narrow(column, carry):
        at = pl.ds(column * pitch, rows)
        for half in range(halves):
            stage_ref[column, :, half * LANES : (half + 1) * LANES] = wide_ref[half, at, :].astype(
                BF16
            )
        return carry

    for n in range(chunks):
        lax.fori_loop(n * width, (n + 1) * width, narrow, 0, unroll=4)
        copies[n].start()
    for copy in copies:
        copy.wait()


def on_device(tracers, wind_fields, departures):
    columns, rows, tracer_ch = tracers.shape
    levels = wind_fields.shape[-1] // 4
    per_level = tracer_ch // levels
    bands = departures.shape[1]
    band_rows = rows // bands
    inner = columns * levels // LANES
    padded_inner = -(-(inner + 2 * RIM) // 8) * 8
    size = band_rows * inner
    offsets = LAST - FIRST
    halves = tracer_ch // LANES
    rim_at = CAP * 2 * size + META
    rim_rows = (RIM * halves + 1) * rows

    wide = per_level * LANES
    table = jnp.transpose(departures, (0, 2, 1))

    vmem = pl.BlockSpec(memory_space=pltpu.VMEM)
    smem = pl.BlockSpec(memory_space=pltpu.SMEM)
    hbm = pl.BlockSpec(memory_space=pltpu.HBM)
    tables = [pltpu.SMEM((offsets * CAP,), jnp.int32), pltpu.SMEM((offsets,), jnp.int32)]

    def params(mib):
        return pltpu.CompilerParams(vmem_limit_bytes=mib << 20)

    *messages, spread, join = pl.pallas_call(
        functools.partial(wind_kernel, (columns, rows, inner, bands, band_rows)),
        out_shape=[
            jax.ShapeDtypeStruct((rim_at + (rim_rows if abs(n) == 1 else 0), LANES), BF16)
            for n in range(FIRST, LAST)
        ]
        + [jax.ShapeDtypeStruct((wide, wide), BF16)] * 2,
        in_specs=[hbm] * 3,
        out_specs=[vmem] * (offsets + 2),
        scratch_shapes=[
            pltpu.SMEM(table.shape, jnp.int32),
            pltpu.VMEM(wind_fields.shape, BF16),
            pltpu.VMEM((columns * (rows + 1), LANES), F32),
            pltpu.VMEM((2, rows, inner, LANES), F32),
            pltpu.VMEM((columns // inner * LANES, 2 * LANES), BF16),
            pltpu.VMEM((2, RIM, rows, tracer_ch), BF16),
            pltpu.SemaphoreType.DMA((3,)),
            pltpu.SemaphoreType.DMA((columns // inner,)),
        ]
        + tables,
        compiler_params=params(16),
        cost_estimate=pl.CostEstimate(flops=4_000_000, bytes_accessed=3_000_000, transcendentals=0),
        name="winds",
    )(*(pltpu.with_memory_space_constraint(x, pltpu.HBM) for x in (table, wind_fields, tracers)))

    arrived = {}
    for n in ORDER:
        msg = messages[n - FIRST]
        arrived[n] = msg if n == 0 else shifted(msg, "lon", -n)

    all_rows = (columns - inner + padded_inner) * (rows + 1)
    prepare = pl.pallas_call(
        functools.partial(prepare_kernel, (columns, rows, inner, padded_inner, rim_at)),
        out_shape=[
            jax.ShapeDtypeStruct((per_level, rows + 2 * RIM + 1, padded_inner, LANES), F32),
            jax.ShapeDtypeStruct((2, rows + 2 * RIM + 1, padded_inner, LANES), F32),
        ],
        in_specs=[vmem] * 5,
        out_specs=[vmem] * 2,
        scratch_shapes=[
            pltpu.VMEM((halves, all_rows, LANES), F32),
            pltpu.VMEM((all_rows, LANES), F32),
            pltpu.VMEM((columns // inner * LANES, 4 * LANES), BF16),
        ],
        compiler_params=params(32),
        cost_estimate=pl.CostEstimate(
            flops=16_000_000, bytes_accessed=12_000_000, transcendentals=0
        ),
        name="prepare",
    )
    fields, extra = prepare(tracers, wind_fields, arrived[-1], arrived[1], spread)

    advect = pl.pallas_call(
        functools.partial(advect_kernel, (inner, band_rows)),
        out_shape=jax.ShapeDtypeStruct((CAP * size, wide), BF16),
        in_specs=[vmem] * 4,
        out_specs=vmem,
        scratch_shapes=[
            pltpu.VMEM((CAP * size, wide), F32),
            pltpu.SMEM((CAP,), jnp.int32),
        ],
        compiler_params=params(12),
        cost_estimate=pl.CostEstimate(
            flops=16_000_000, bytes_accessed=6_000_000, transcendentals=0
        ),
        name="advect",
    )
    received = [None] * offsets
    for n in ORDER:
        result = advect(arrived[n], fields, extra, join)
        received[n - FIRST] = result if n == 0 else shifted(result, "lon", n)

    sizes = (columns, rows, inner, bands, band_rows)
    wide_shape = jax.ShapeDtypeStruct((halves, columns * (rows + 1), LANES), F32)
    early = ORDER[: offsets - 1 - LATE] + ORDER[-1:]
    late = ORDER[offsets - 1 - LATE : -1]
    first = pl.pallas_call(
        functools.partial(early_kernel, sizes, early),
        out_shape=[wide_shape, jax.ShapeDtypeStruct((offsets * CAP,), jnp.int32)],
        in_specs=[smem] + [vmem] * len(early),
        out_specs=[vmem, smem],
        scratch_shapes=tables[1:],
        compiler_params=params(8),
        cost_estimate=pl.CostEstimate(flops=2_000_000, bytes_accessed=6_000_000, transcendentals=0),
        name="early",
    )
    spread_out, slots = first(table, *[received[n - FIRST] for n in early])
    last = pl.pallas_call(
        functools.partial(late_kernel, sizes, late),
        out_shape=[jax.ShapeDtypeStruct((columns, rows, tracer_ch), BF16), wide_shape],
        in_specs=[smem] + [vmem] * (len(late) + 1),
        out_specs=[pl.BlockSpec(memory_space=pl.ANY), vmem],
        scratch_shapes=[
            pltpu.VMEM((columns, rows, tracer_ch), BF16),
            pltpu.SemaphoreType.DMA((8,)),
        ],
        input_output_aliases={len(late) + 1: 1},
        compiler_params=params(8),
        cost_estimate=pl.CostEstimate(flops=2_000_000, bytes_accessed=6_000_000, transcendentals=0),
        name="late",
    )
    return last(slots, *[received[n - FIRST] for n in late], spread_out)[0]


def solution(mesh):
    placed = (
        P(("groups", "lon"), None, None),
        P(("groups", "lon"), None, None),
        P(("groups", "lon"), None, None),
    )
    return jax.shard_map(
        on_device,
        mesh=mesh,
        in_specs=placed,
        out_specs=P(("groups", "lon"), None, None),
        check_vma=False,
    )
```
